128 devices in a mesh: vocab: 32 (over y, x, core), dp: 4 (over z).
Axes of the slice: x: 4, y: 4, z: 4, core: 2. Of those that a mesh axis runs over, the one named last changes fastest.
Arguments:
- token_ids: int32 [131072], P(('vocab', 'dp')), may hold values from 0 to 1048575, as said below
- counts: int32 [128], P(('vocab', 'dp')), may hold values from 256 to 1024, as said below
- table: bfloat16 [1048576, 128], P(('vocab', 'dp')), may hold values from -6 to 6
- projection: bfloat16 [128, 4096], replicated, may hold values from -0.5 to 0.5
- cotangent: bfloat16 [131072, 4096], P(('vocab', 'dp')), may hold values from -4 to 4
Outputs:
- hidden: bfloat16 [131072, 4096], P(('vocab', 'dp'))
- grad_projection: float32 [128, 4096], replicated
- grad_table: float32 [1048576, 128], P(('vocab', 'dp'))
The draws below stay inside these ranges and needn't reach their ends.
Inputs may be any that keep to these rules, and one draw needn't show every extreme that they name: `token_ids`: on each device at most 16 tokens have ids in the rows of any one device, and in every draw one device's rows receive exactly 16 tokens from every device; which rows are frequent is drawn from the seed. `counts`: in every draw some device has all 1024 tokens live.
All inputs are finite; a program needn't handle non-finite values.
Results may differ from the reference program's by a relative error of at most 0.0029.
Values may be sent and summed in bfloat16 or wider, within the bound.
No kernel may reach another device: no remote copies, remote signals or barrier semaphores. Data moves between devices by JAX's collectives and lax.ppermute only.
A program may use at most 128 MiB of HBM per device.

```python
import jax
import jax.numpy as jnp
from jax import lax

E = 128
H = 4096
V_DEV = 8192
TOK_DEV = 1024
VOCAB = 1048576
TOKENS = 131072
CAP = 16
DEVICES = 128


def draw_token_ids(key, part):
    base = jax.random.fold_in(key, 11)
    hot_owner = jax.random.randint(jax.random.fold_in(base, 1), (), 0, DEVICES)
    owner_shift = jax.random.randint(jax.random.fold_in(base, 2), (DEVICES,), 0, 7)
    row_mult = 2 * jax.random.randint(jax.random.fold_in(base, 3), (), 0, 16384) + 1
    row_add = jax.random.randint(jax.random.fold_in(base, 4), (), 0, V_DEV)
    slots = DEVICES * CAP
    slot_place = jnp.arange(slots, dtype=jnp.int32)
    slot_owner = slot_place // CAP

    def one_device(device):
        inner = jax.random.fold_in(base, 100 + device)
        first, second, third, fourth = jax.random.split(inner, 4)
        raw = jax.random.randint(first, (slots,), 0, 65536)
        score = (raw >> owner_shift[slot_owner]) * slots + slot_place
        score = score + jnp.where(slot_owner == hot_owner, 1 << 29, 0)
        picked = lax.top_k(score, TOK_DEV)[1]
        owner = picked // CAP
        start = jax.random.randint(second, (TOK_DEV,), 0, V_DEV)
        shifts = jax.random.randint(third, (TOK_DEV,), 0, 9)
        local_row = ((start >> shifts) * row_mult + row_add) % V_DEV
        identity = owner * V_DEV + local_row
        order = jax.random.permutation(fourth, TOK_DEV)
        return identity[order].astype(jnp.int32)
    return jax.vmap(one_device)(jnp.arange(DEVICES, dtype=jnp.int32)).reshape(-1)


def draw_counts(key, part):
    drawn = jax.random.randint(jax.random.fold_in(key, 21), (DEVICES,), TOK_DEV // 4, TOK_DEV + 1)
    full_device = jax.random.randint(jax.random.fold_in(key, 22), (), 0, DEVICES)
    return jnp.where(jnp.arange(DEVICES) == full_device, TOK_DEV, drawn).astype(jnp.int32)


def shard_levels(key, dims, cuts, low, top_value):
    level, own = 1.0, jax.random.fold_in(key, 6)
    for axis_at, parts in cuts:
        steps = jnp.exp(jax.random.uniform(jax.random.fold_in(own, axis_at), (parts,), jnp.float32, low / len(cuts), top_value / len(cuts)))
        level = level * jnp.repeat(steps, dims[axis_at] // parts).reshape([-1 if axis == axis_at else 1 for axis in range(len(dims))])
    return level


def normal_values(rng, dims, width, bound, shards=(), held_as=jnp.bfloat16):
    entries = width * jax.random.normal(rng, dims, jnp.float32)
    if shards:
        entries = entries * shard_levels(rng, dims, shards, -0.22, 0.18)
    return jnp.clip(entries, -bound, bound).astype(held_as)


def setup_inputs(seed: int = 0) -> dict:
    streams_of = jax.random.split(jax.random.key(seed), 6)
    token_ids = draw_token_ids(jax.random.fold_in(streams_of[5], 71), 0)
    counts = draw_counts(jax.random.fold_in(streams_of[5], 71), 0)
    table = normal_values(streams_of[2], (VOCAB, E), 1.0, 6.0, ((0, 128),))
    projection = normal_values(streams_of[3], (E, H), E ** -0.5, 0.5)
    cotangent = normal_values(streams_of[4], (TOKENS, H), 0.25, 4.0, ((0, 128),))
    return {"token_ids": token_ids, "counts": counts, "table": table, "projection": projection, "cotangent": cotangent}


def reference(token_ids, counts, table, projection, cotangent):
    position = jnp.arange(TOKENS, dtype=jnp.int32)
    holder = position // TOK_DEV
    live = (position - holder * TOK_DEV) < counts[holder]
    embedded = table[token_ids]
    product = jnp.dot(embedded, projection, preferred_element_type=jnp.float32)
    hidden = jnp.where(live[:, None], product, 0.0).astype(jnp.bfloat16)
    masked = jnp.where(live[:, None], cotangent, jnp.zeros_like(cotangent))
    terms = lax.dot_general(embedded, masked, (((0,), (0,)), ((), ())), preferred_element_type=jnp.float32)
    grad_projection = terms * (1.0 / (TOKENS ** 0.5))
    token_grad = lax.dot_general(masked, projection, (((1,), (1,)), ((), ())), preferred_element_type=jnp.float32).astype(jnp.bfloat16)
    grad_table = jax.ops.segment_sum(token_grad.astype(jnp.float32), token_ids, num_segments=VOCAB)
    return hidden, grad_projection, grad_table
```

```python
import functools
import math

import jax
import jax.numpy as jnp
from jax import lax
from jax.experimental import pallas as pl
from jax.experimental.pallas import tpu as pltpu
from jax.sharding import Mesh
from jax.sharding import PartitionSpec as P


ALL = ("vocab_0", "vocab_1", "vocab_2", "dp")
CHIPS = ("vocab_0", "vocab_1", "dp")
CORE = "vocab_2"
SWAP = ((0, 1), (1, 0))
LANES = 128
BF16 = jnp.bfloat16
F32 = jnp.float32
VMEM = pl.BlockSpec(memory_space=pltpu.VMEM)
SMEM = pl.BlockSpec(memory_space=pltpu.SMEM)
HBM = pl.BlockSpec(memory_space=pltpu.HBM)


def in_hbm(x):
    return pltpu.with_memory_space_constraint(x, pltpu.HBM)


def in_vmem(x):
    return pltpu.with_memory_space_constraint(x, pltpu.VMEM)


def params(mib):
    return pltpu.CompilerParams(vmem_limit_bytes=mib << 20)


def cost(flops, nbytes):
    return pl.CostEstimate(flops=flops, bytes_accessed=nbytes, transcendentals=0)


def dot(a, b, dims=((1,), (0,))):
    return lax.dot_general(a, b, (dims, ((), ())), preferred_element_type=F32)


def one_hot(hit):
    return jnp.where(hit, 1.0, 0.0).astype(BF16)


def exchange(blocks, axes):
    return lax.all_to_all(blocks, axes, split_axis=0, concat_axis=0, tiled=True)


def front_kernel(
    shift, capacity, count_ref, ids_ref, proj_hbm, cot_hbm, slot_ref, out_ref, cot, proj, across, grads, sems
):
    tokens, _ = cot.shape
    steps = slot_ref.shape[0]
    block = tokens // steps
    proj_copy = pltpu.make_async_copy(proj_hbm, proj, sems.at[steps])
    proj_copy.start()
    copies = []
    for i in range(steps):
        rows = pl.ds(i * block, block)
        copies.append(pltpu.make_async_copy(cot_hbm.at[rows, :], cot.at[rows, :], sems.at[i]))
        copies[-1].start()

    ids = ids_ref[...]
    owner = lax.shift_right_logical(ids, shift)
    row = ids & ((1 << shift) - 1)
    chunks, lanes = ids.shape
    n = out_ref.shape[0] // (capacity + 2)
    holder = lax.broadcasted_iota(jnp.int32, (n, lanes), 0)
    before = one_hot(
        lax.broadcasted_iota(jnp.int32, (lanes, lanes), 0)
        < lax.broadcasted_iota(jnp.int32, (lanes, lanes), 1)
    )
    place = lax.broadcasted_iota(jnp.int32, (LANES, lanes), 0)
    seen = jnp.zeros((n, 1), F32)
    high = jnp.zeros((n, LANES), F32)
    low = jnp.zeros((n, LANES), F32)
    targets = []
    for k in range(chunks):
        own = owner[k : k + 1, :]
        hit = holder == own
        hits = one_hot(hit)
        earlier = dot(hits, before) + seen
        rank = jnp.sum(jnp.where(hit, earlier, 0.0), axis=0, keepdims=True).astype(jnp.int32)
        seen = seen + jnp.sum(jnp.where(hit, 1.0, 0.0), axis=1, keepdims=True)
        per = block // lanes
        slot_ref[k // per, :, (k % per) * lanes : (k % per + 1) * lanes] = own * capacity + rank
        targets.append(own * (capacity + 2) + rank)
        mine = place == rank
        line = row[k : k + 1, :]
        upper = lax.shift_right_logical(line, 7).astype(F32)
        lower = (line & 127).astype(F32)
        high = high + dot(hits, jnp.where(mine, upper, 0.0).astype(BF16), ((1,), (1,)))
        low = low + dot(hits, jnp.where(mine, lower, 0.0).astype(BF16), ((1,), (1,)))
    last = lax.broadcasted_iota(jnp.int32, (1, n), 1) * (capacity + 2) + capacity
    targets += [last, last + 1]
    grads[tokens : tokens + n, :] = high.astype(BF16)
    grads[tokens + n : tokens + 2 * n, :] = low.astype(BF16)

    proj_copy.wait()
    across[...] = proj[...].T
    for i in range(steps):
        copies[i].wait()
        rows = slice(i * block, (i + 1) * block)
        grad = dot(cot[rows, :], across[...])
        token = lax.broadcasted_iota(jnp.int32, grad.shape, 0) + i * block
        grads[rows, :] = jnp.where(token < count_ref[0], grad, 0.0).astype(BF16)

    step = 256
    line = lax.broadcasted_iota(jnp.int32, (step, lanes), 0)
    for c in range(out_ref.shape[0] // step):
        total = jnp.zeros((step, out_ref.shape[1]), F32)
        for k in range(0, len(targets), 2):
            left = one_hot(line == targets[k] - c * step)
            right = one_hot(line == targets[k + 1] - c * step)
            total += dot(
                jnp.concatenate([left, right], axis=1), grads[k * lanes : (k + 2) * lanes, :]
            )
        out_ref[c * step : (c + 1) * step, :] = total.astype(BF16)


def front(counts, token_ids, projection, cotangent, held_rows, n, capacity, block):
    tokens, hidden = cotangent.shape
    width = projection.shape[0]
    shift = held_rows.bit_length() - 1
    assert held_rows == 1 << shift and shift <= 15 and n == width == LANES
    rows = n * (capacity + 2)
    return pl.pallas_call(
        functools.partial(front_kernel, shift, capacity),
        out_shape=(
            jax.ShapeDtypeStruct((tokens // block, 1, block), jnp.int32),
            jax.ShapeDtypeStruct((rows, width), BF16),
        ),
        in_specs=[SMEM, VMEM, HBM, HBM],
        out_specs=(VMEM, VMEM),
        scratch_shapes=[
            pltpu.VMEM((tokens, hidden), BF16),
            pltpu.VMEM((width, hidden), BF16),
            pltpu.VMEM((hidden, width), BF16),
            pltpu.VMEM((tokens + 2 * n, width), BF16),
            pltpu.SemaphoreType.DMA((tokens // block + 1,)),
        ],
        compiler_params=params(24),
        cost_estimate=cost(3 << 29, 10 << 20),
        name="front",
    )(counts, token_ids.reshape(tokens // LANES, LANES), in_hbm(projection), in_hbm(cotangent))


def hold_kernel(table_hbm, out_ref, sem):
    copy = pltpu.make_async_copy(table_hbm, out_ref, sem)
    copy.start()
    copy.wait()


def held_table(table):
    return pl.pallas_call(
        hold_kernel,
        out_shape=pltpu.VMEM(table.shape, table.dtype),
        in_specs=[HBM],
        out_specs=VMEM,
        scratch_shapes=[pltpu.SemaphoreType.DMA(())],
        compiler_params=params(4),
        cost_estimate=cost(1 << 22, 6 << 20),
        name="held_table",
    )(in_hbm(table))


def pick_kernel(capacity, arrived_ref, table_ref, out_ref, index_ref, wide, index, table, stage, sem):
    wide[...] = arrived_ref[...].astype(F32)
    n = index_ref.shape[1]
    high = wide[pl.ds(capacity, n, stride=capacity + 2), :]
    low = wide[pl.ds(capacity + 1, n, stride=capacity + 2), :]
    rows = (high * 128.0 + low).T
    index_ref[...] = rows[:capacity, :].astype(jnp.int32)
    copy = pltpu.make_async_copy(index_ref, index, sem)
    copy.start()
    step = 256

    @pl.loop(0, table_ref.shape[0] // step)
    def _(c):
        part = pl.ds(pl.multiple_of(c * step, step), step)
        table[part, :] = table_ref[part, :].astype(F32)

    copy.wait()
    unroll = 4

    @pl.loop(0, n // unroll)
    def _(q):
        for k in range(unroll):
            p = q * unroll + k
            for r in range(capacity):
                stage[pl.ds(p * capacity + r, 1), :] = table[pl.ds(index[r, p], 1), :]

    out_ref[...] = stage[...].astype(BF16)


def picked_rows(arrived, table, n, capacity):
    rows, width = arrived.shape
    slots = n * capacity
    return pl.pallas_call(
        functools.partial(pick_kernel, capacity),
        out_shape=(
            jax.ShapeDtypeStruct((slots, width), BF16),
            jax.ShapeDtypeStruct((capacity, n), jnp.int32),
        ),
        in_specs=[VMEM, VMEM],
        out_specs=(VMEM, VMEM),
        scratch_shapes=[
            pltpu.VMEM((rows, width), F32),
            pltpu.SMEM((capacity, n), jnp.int32),
            pltpu.VMEM(table.shape, F32),
            pltpu.VMEM((slots, width), F32),
            pltpu.SemaphoreType.DMA(()),
        ],
        compiler_params=params(12),
        cost_estimate=cost(1 << 26, 3 << 20),
        name="picked_rows",
    )(arrived, table)


def rows_sum_kernel(capacity, index_ref, grads_ref, out_ref, wide, first, second, third):
    sums = (out_ref, first, second, third)
    step = 256

    @pl.loop(0, out_ref.shape[0] // step)
    def _(c):
        rows = pl.ds(pl.multiple_of(c * step, step), step)
        for total in sums:
            total[rows, :] = jnp.zeros((step, out_ref.shape[1]), F32)

    wide[...] = grads_ref[...].astype(F32)
    n = index_ref.shape[1]
    quarter = n // len(sums)

    @pl.loop(0, quarter)
    def _(q):
        for r in range(capacity):
            for s, total in enumerate(sums):
                p = q + s * quarter
                row = pl.ds(index_ref[r, p], 1)
                total[row, :] += wide[pl.ds(p * (capacity + 2) + r, 1), :]

    @pl.loop(0, out_ref.shape[0] // step)
    def _(c):
        rows = pl.ds(pl.multiple_of(c * step, step), step)
        out_ref[rows, :] = (out_ref[rows, :] + first[rows, :]) + (second[rows, :] + third[rows, :])


def rows_sum(index, arrived, held_rows, capacity):
    rows, width = arrived.shape
    return pl.pallas_call(
        functools.partial(rows_sum_kernel, capacity),
        out_shape=jax.ShapeDtypeStruct((held_rows, width), F32),
        in_specs=[SMEM, VMEM],
        out_specs=VMEM,
        scratch_shapes=[
            pltpu.VMEM((rows, width), F32),
            pltpu.VMEM((held_rows, width), F32),
            pltpu.VMEM((held_rows, width), F32),
            pltpu.VMEM((held_rows, width), F32),
        ],
        compiler_params=params(24),
        cost_estimate=cost(1 << 28, 6 << 20),
        name="rows_sum",
    )(index, arrived)


def cot_copies(half_ref, cot_hbm, cot, sems):
    tokens, wide = cot.shape
    steps = sems.shape[0]
    block = tokens // steps
    columns = pl.ds(pl.multiple_of(half_ref[0] * wide, wide), wide)
    copies = []
    for i in range(steps):
        rows = pl.ds(i * block, block)
        copies.append(
            pltpu.make_async_copy(cot_hbm.at[rows, columns], cot.at[rows, :], sems.at[i])
        )
        copies[-1].start()
    return copies


def half_product(emb_ref, cot, copies, out_ref):
    block = 512
    for copy in copies:
        copy.wait()
    for i in range(out_ref.shape[1] // block):
        columns = slice(i * block, (i + 1) * block)
        out_ref[:, columns] = dot(emb_ref[...], cot[:, columns])


def terms_kernel(half_ref, emb_ref, cot_hbm, out_ref, cot, sems):
    copies = cot_copies(half_ref, cot_hbm, cot, sems)
    half_product(emb_ref, cot, copies, out_ref)


def first_terms_kernel(
    half_ref, count_ref, slot_ref, rows_ref, cot_hbm, emb_ref, out_ref, cot, sems
):
    copies = cot_copies(half_ref, cot_hbm, cot, sems)
    across = rows_ref[...].T
    chunks, _, block = slot_ref.shape
    step = 256
    for k in range(chunks):
        slot = slot_ref[k]
        total = jnp.zeros((across.shape[0], block), F32)
        line = lax.broadcasted_iota(jnp.int32, (step, block), 0)
        for c in range(across.shape[1] // step):
            total += dot(across[:, c * step : (c + 1) * step], one_hot(line + c * step == slot))
        token = lax.broadcasted_iota(jnp.int32, total.shape, 1) + k * block
        total = jnp.where(token < count_ref[0], total, 0.0)
        emb_ref[:, k * block : (k + 1) * block] = total.astype(BF16)
    half_product(emb_ref, cot, copies, out_ref)


def first_terms(half, counts, slots, returned, cotangent):
    tokens, hidden = cotangent.shape
    width = returned.shape[1]
    return pl.pallas_call(
        first_terms_kernel,
        in_specs=[SMEM, SMEM, VMEM, VMEM, HBM],
        out_specs=(VMEM, VMEM),
        scratch_shapes=[
            pltpu.VMEM((tokens, hidden // 2), BF16),
            pltpu.SemaphoreType.DMA((4,)),
        ],
        out_shape=(
            jax.ShapeDtypeStruct((width, tokens), BF16),
            jax.ShapeDtypeStruct((width, hidden // 2), F32),
        ),
        compiler_params=params(16),
        cost_estimate=cost(3 << 28, 6 << 20),
        name="first_terms",
    )(half, counts, slots, returned, in_hbm(cotangent))


def half_terms(half, embedded, cotangent):
    tokens, hidden = cotangent.shape
    width = embedded.shape[0]
    return pl.pallas_call(
        terms_kernel,
        in_specs=[SMEM, VMEM, HBM],
        out_specs=VMEM,
        scratch_shapes=[
            pltpu.VMEM((tokens, hidden // 2), BF16),
            pltpu.SemaphoreType.DMA((4,)),
        ],
        out_shape=jax.ShapeDtypeStruct((width, hidden // 2), F32),
        compiler_params=params(16),
        cost_estimate=cost(1 << 29, 5 << 20),
        name="half_terms",
    )(half, embedded, in_hbm(cotangent))


def parts_kernel(tiles, mine_ref, other_ref, out_ref):
    groups = mine_ref.shape[1] // (tiles * LANES)
    for g in range(mine_ref.shape[0] // 8):
        rows = slice(8 * g, 8 * g + 8)
        for j in range(groups):
            columns = slice(j * tiles * LANES, (j + 1) * tiles * LANES)
            total = mine_ref[rows, columns] + other_ref[rows, columns]
            block = [total[:, t * LANES : (t + 1) * LANES] for t in range(tiles)]
            out_ref[g * groups + j] = jnp.concatenate(block, axis=0).astype(BF16)


def chip_parts(mine, other, chips):
    rows, columns = mine.shape
    tiles = rows * columns // (8 * LANES * chips)
    return pl.pallas_call(
        functools.partial(parts_kernel, tiles),
        out_shape=jax.ShapeDtypeStruct((chips, 8 * tiles, LANES), BF16),
        in_specs=[VMEM, VMEM],
        out_specs=VMEM,
        compiler_params=params(8),
        cost_estimate=cost(1 << 24, 3 << 20),
        name="chip_parts",
    )(mine, other)


def total_kernel(parts_ref, out_ref):
    total = parts_ref[0].astype(F32)
    for p in range(1, parts_ref.shape[0]):
        total += parts_ref[p].astype(F32)
    total = total.astype(BF16)
    for p in range(out_ref.shape[0]):
        out_ref[p] = total


def chips_total(parts):
    return pl.pallas_call(
        total_kernel,
        out_shape=jax.ShapeDtypeStruct(parts.shape, BF16),
        in_specs=[VMEM],
        out_specs=VMEM,
        compiler_params=params(8),
        cost_estimate=cost(1 << 24, 1 << 20),
        name="chips_total",
    )(parts)


def result_kernel(tiles, scaling, core_ref, mine_ref, other_ref, out_ref):
    half = out_ref.shape[1] // 2
    groups = half // (tiles * LANES)
    for side in range(2):
        for source, core in ((mine_ref, side), (other_ref, 1 - side)):

            @pl.when(core_ref[0] == core)
            def _():
                for g in range(out_ref.shape[0] // 8):
                    for j in range(groups):
                        block = source[g * groups + j].astype(F32) * scaling
                        for t in range(tiles):
                            left = side * half + (j * tiles + t) * LANES
                            out_ref[8 * g : 8 * g + 8, left : left + LANES] = block[
                                8 * t : 8 * t + 8, :
                            ]


def result(core, mine, other, width, hidden, scaling):
    tiles = mine.shape[1] // 8
    return pl.pallas_call(
        functools.partial(result_kernel, tiles, scaling),
        out_shape=jax.ShapeDtypeStruct((width, hidden), F32),
        in_specs=[SMEM, VMEM, VMEM],
        out_specs=VMEM,
        compiler_params=params(8),
        cost_estimate=cost(1 << 24, 3 << 20),
        name="result",
    )(core, mine, other)


def hidden_kernel(emb_ref, proj_ref, out_ref):
    out_ref[...] = dot(emb_ref[...].T, proj_ref[...]).astype(BF16)


def hidden_rows(embedded, projection):
    width, tokens = embedded.shape
    hidden = projection.shape[1]
    block = 256
    return pl.pallas_call(
        hidden_kernel,
        grid=(tokens // block,),
        out_shape=jax.ShapeDtypeStruct((tokens, hidden), BF16),
        in_specs=[
            pl.BlockSpec((width, block), lambda i: (0, i)),
            pl.BlockSpec((width, hidden), lambda i: (0, 0)),
        ],
        out_specs=pl.BlockSpec((block, hidden), lambda i: (i, 0)),
        compiler_params=params(16),
        cost_estimate=cost(1 << 30, 9 << 20),
        name="hidden_rows",
    )(embedded, projection)


def body(token_ids, counts, table, projection, cotangent):
    tokens = token_ids.shape[0]
    held_rows, width = table.shape
    hidden_width = projection.shape[1]
    n = lax.axis_size(ALL)
    chips = lax.axis_size(CHIPS)
    capacity = 2 * tokens // n
    core = lax.axis_index(CORE).astype(jnp.int32).reshape(1)
    slots, outgoing = front(counts, token_ids, projection, cotangent, held_rows, n, capacity, 256)
    incoming = exchange(outgoing.reshape(n, -1, 2, width), ALL).reshape(-1, width)
    held = held_table(table)
    picked, index = picked_rows(incoming, in_vmem(held), n, capacity)
    returned = exchange(picked.reshape(n, capacity, width), ALL).reshape(-1, width)
    embedded, theirs = first_terms(1 - core, counts, slots, returned, cotangent)
    other = lax.ppermute(theirs, CORE, SWAP)
    mine = half_terms(core, embedded, cotangent)
    parts = chip_parts(mine, other, chips)
    arrived = exchange(parts, CHIPS)
    hidden = hidden_rows(embedded, projection)
    total = chips_total(arrived)
    whole = exchange(total, CHIPS)
    across = lax.ppermute(whole, CORE, SWAP)
    scaling = 1.0 / math.sqrt(tokens * n)
    grad_projection = result(core, whole, across, width, hidden_width, scaling)
    grad_table = rows_sum(index, incoming, held_rows, capacity)
    return (hidden, grad_projection, grad_table)


def solution(mesh):
    finer = Mesh(
        mesh.devices.reshape(4, 4, 2, mesh.shape["dp"]), ("vocab_0", "vocab_1", "vocab_2", "dp")
    )
    in_specs = (P(ALL), P(ALL), P(ALL, None), P(), P(ALL, None))
    out_specs = (P(ALL, None), P(), P(ALL, None))
    return jax.shard_map(body, mesh=finer, in_specs=in_specs, out_specs=out_specs, check_vma=False)
```

```python
import functools
import math

import jax
import jax.numpy as jnp
from jax import lax
from jax.experimental import pallas as pl
from jax.experimental.pallas import tpu as pltpu
from jax.sharding import Mesh
from jax.sharding import PartitionSpec as P


ALL = ("vocab_0", "vocab_1", "vocab_2", "dp")
CHIPS = ("vocab_0", "vocab_1", "dp")
CORE = "vocab_2"
SWAP = ((0, 1), (1, 0))
LANES = 128
BF16 = jnp.bfloat16
F32 = jnp.float32
VMEM = pl.BlockSpec(memory_space=pltpu.VMEM)
SMEM = pl.BlockSpec(memory_space=pltpu.SMEM)
HBM = pl.BlockSpec(memory_space=pltpu.HBM)


def in_hbm(x):
    return pltpu.with_memory_space_constraint(x, pltpu.HBM)


def in_vmem(x):
    return pltpu.with_memory_space_constraint(x, pltpu.VMEM)


def params(mib):
    return pltpu.CompilerParams(vmem_limit_bytes=mib << 20)


def cost(flops, nbytes):
    return pl.CostEstimate(flops=flops, bytes_accessed=nbytes, transcendentals=0)


def dot(a, b, dims=((1,), (0,))):
    return lax.dot_general(a, b, (dims, ((), ())), preferred_element_type=F32)


def one_hot(hit):
    return jnp.where(hit, 1.0, 0.0).astype(BF16)


def exchange(blocks, axes):
    return lax.all_to_all(blocks, axes, split_axis=0, concat_axis=0, tiled=True)


def prepare_kernel(shift, capacity, core_ref, count_ref, ids_ref, slot_ref, request_ref):
    del core_ref, count_ref
    n = request_ref.shape[0]
    chunks, lanes = ids_ref.shape
    holder = lax.broadcasted_iota(jnp.int32, (n, lanes), 0)
    before = one_hot(
        lax.broadcasted_iota(jnp.int32, (lanes, lanes), 0)
        < lax.broadcasted_iota(jnp.int32, (lanes, lanes), 1)
    )
    place = lax.broadcasted_iota(jnp.int32, (capacity, lanes), 0)
    seen = jnp.zeros((n, 1), F32)
    high = jnp.zeros((n, capacity), F32)
    low = jnp.zeros((n, capacity), F32)
    ids = ids_ref[...]
    owner = lax.shift_right_logical(ids, shift)
    row = ids & ((1 << shift) - 1)
    for k in range(chunks):
        own = owner[k : k + 1, :]
        hit = holder == own
        hits = one_hot(hit)
        earlier = dot(hits, before) + seen
        rank = jnp.sum(jnp.where(hit, earlier, 0.0), axis=0, keepdims=True).astype(jnp.int32)
        seen = seen + jnp.sum(jnp.where(hit, 1.0, 0.0), axis=1, keepdims=True)
        per = slot_ref.shape[2] // lanes
        slot_ref[k // per, :, (k % per) * lanes : (k % per + 1) * lanes] = own * capacity + rank
        mine = place == rank
        line = row[k : k + 1, :]
        upper = lax.shift_right_logical(line, 7).astype(F32)
        lower = (line & 127).astype(F32)
        high = high + dot(hits, jnp.where(mine, upper, 0.0).astype(BF16), ((1,), (1,)))
        low = low + dot(hits, jnp.where(mine, lower, 0.0).astype(BF16), ((1,), (1,)))
    request_ref[...] = (high * 128.0 + low).astype(jnp.int32)


def prepare(core, counts, token_ids, held_rows, n, capacity, block):
    tokens = token_ids.shape[0]
    shift = held_rows.bit_length() - 1
    assert held_rows == 1 << shift and shift <= 15
    return pl.pallas_call(
        functools.partial(prepare_kernel, shift, capacity),
        out_shape=(
            jax.ShapeDtypeStruct((tokens // block, 1, block), jnp.int32),
            jax.ShapeDtypeStruct((n, capacity), jnp.int32),
        ),
        in_specs=[SMEM, SMEM, VMEM],
        out_specs=(VMEM, VMEM),
        compiler_params=params(8),
        cost_estimate=cost(1 << 26, 1 << 16),
        name="prepare",
    )(core, counts, token_ids.reshape(tokens // LANES, LANES))


def grads_kernel(
    count_ref, slot_ref, proj_hbm, cot_hbm, table_hbm, out_ref, table, cot, proj, across, grads, sems
):
    steps, _, block = slot_ref.shape
    proj_copy = pltpu.make_async_copy(proj_hbm, proj, sems.at[steps])
    proj_copy.start()
    copies = []
    for i in range(steps):
        rows = pl.ds(i * block, block)
        copies.append(pltpu.make_async_copy(cot_hbm.at[rows, :], cot.at[rows, :], sems.at[i]))
        copies[-1].start()
    table_copy = pltpu.make_async_copy(table_hbm, table, sems.at[steps + 1])
    table_copy.start()
    proj_copy.wait()
    across[...] = proj[...].T
    for i in range(steps):
        copies[i].wait()
        rows = slice(i * block, (i + 1) * block)
        grad = dot(cot[rows, :], across[...])
        token = lax.broadcasted_iota(jnp.int32, grad.shape, 0) + i * block
        grads[rows, :] = jnp.where(token < count_ref[0], grad, 0.0).astype(BF16)
    step = 256
    line = lax.broadcasted_iota(jnp.int32, (step, block), 0)
    for c in range(out_ref.shape[0] // step):
        total = jnp.zeros((step, out_ref.shape[1]), F32)
        for k in range(steps):
            hit = line == slot_ref[k] - c * step
            total += dot(one_hot(hit), grads[k * block : (k + 1) * block, :])
        out_ref[c * step : (c + 1) * step, :] = total.astype(BF16)
    table_copy.wait()


def placed_grads(counts, slots, projection, cotangent, table, n_slots):
    tokens, hidden = cotangent.shape
    width = projection.shape[0]
    return pl.pallas_call(
        grads_kernel,
        out_shape=(
            jax.ShapeDtypeStruct((n_slots, width), BF16),
            pltpu.VMEM(table.shape, table.dtype),
        ),
        in_specs=[SMEM, VMEM, HBM, HBM, HBM],
        out_specs=(VMEM, VMEM),
        scratch_shapes=[
            pltpu.VMEM((tokens, hidden), BF16),
            pltpu.VMEM((width, hidden), BF16),
            pltpu.VMEM((hidden, width), BF16),
            pltpu.VMEM((tokens, width), BF16),
            pltpu.SemaphoreType.DMA((slots.shape[0] + 2,)),
        ],
        compiler_params=params(24),
        cost_estimate=cost(3 << 29, 10 << 20),
        name="placed_grads",
    )(counts, slots, in_hbm(projection), in_hbm(cotangent), in_hbm(table))


def pick_kernel(index_ref, grads_ref, held_ref, out_ref, index, table, stage, sem):
    copy = pltpu.make_async_copy(index_ref, index, sem)
    copy.start()
    n, _, capacity = index_ref.shape
    for p in range(n):
        out_ref[p, capacity:, :] = grads_ref[p * capacity : (p + 1) * capacity, :]
    step = 256

    @pl.loop(0, table.shape[0] // step)
    def _(c):
        rows = pl.ds(pl.multiple_of(c * step, step), step)
        table[rows, :] = held_ref[rows, :].astype(F32)

    copy.wait()
    unroll = 4

    @pl.loop(0, n // unroll)
    def _(q):
        for k in range(unroll):
            p = q * unroll + k
            for r in range(capacity):
                stage[pl.ds(p * capacity + r, 1), :] = table[pl.ds(index[p, 0, r], 1), :]

    for p in range(n):
        out_ref[p, :capacity, :] = stage[p * capacity : (p + 1) * capacity, :].astype(BF16)


def picked_rows(received, outgoing, held):
    n, _, capacity = received.shape
    slots = n * capacity
    rows, width = held.shape
    return pl.pallas_call(
        pick_kernel,
        out_shape=jax.ShapeDtypeStruct((n, 2 * capacity, width), BF16),
        in_specs=[VMEM, VMEM, VMEM],
        out_specs=VMEM,
        scratch_shapes=[
            pltpu.SMEM(received.shape, jnp.int32),
            pltpu.VMEM((rows, width), F32),
            pltpu.VMEM((slots, width), F32),
            pltpu.SemaphoreType.DMA(()),
        ],
        compiler_params=params(14),
        cost_estimate=cost(1 << 26, 3 << 20),
        name="picked_rows",
    )(received, outgoing, in_vmem(held))


def rows_sum_kernel(index_ref, grads_ref, out_hbm, index, wide, first, *rest):
    *others, index_sem, sems = rest
    copy = pltpu.make_async_copy(index_ref, index, index_sem)
    copy.start()
    sums = (first, *others)
    held, width = first.shape
    step = 256

    @pl.loop(0, held // step)
    def _(c):
        rows = pl.ds(pl.multiple_of(c * step, step), step)
        for total in sums:
            total[rows, :] = jnp.zeros((step, width), F32)

    n, _, capacity = index_ref.shape
    for p in range(n):
        wide[p * capacity : (p + 1) * capacity, :] = grads_ref[p, capacity:, :].astype(F32)
    copy.wait()
    share = n // len(sums)

    @pl.loop(0, share)
    def _(q):
        for r in range(capacity):
            for s, total in enumerate(sums):
                p = q + s * share
                row = pl.ds(index[p, 0, r], 1)
                total[row, :] += wide[pl.ds(p * capacity + r, 1), :]

    steps = sems.shape[0]
    block = held // steps
    copies = []
    for i in range(steps):

        @pl.loop(i * block // step, (i + 1) * block // step)
        def _(c):
            rows = pl.ds(pl.multiple_of(c * step, step), step)
            first[rows, :] = (first[rows, :] + others[0][rows, :]) + (
                others[1][rows, :] + others[2][rows, :]
            )

        rows = pl.ds(i * block, block)
        copies.append(pltpu.make_async_copy(first.at[rows, :], out_hbm.at[rows, :], sems.at[i]))
        copies[-1].start()
    for copy in copies:
        copy.wait()


def rows_sum(received, arrived, held_rows):
    n, _, capacity = received.shape
    width = arrived.shape[2]
    total = pltpu.VMEM((held_rows, width), F32)
    return pl.pallas_call(
        rows_sum_kernel,
        out_shape=jax.ShapeDtypeStruct((held_rows, width), F32),
        in_specs=[VMEM, VMEM],
        out_specs=HBM,
        scratch_shapes=[
            pltpu.SMEM(received.shape, jnp.int32),
            pltpu.VMEM((n * capacity, width), F32),
            total,
            total,
            total,
            total,
            pltpu.SemaphoreType.DMA(()),
            pltpu.SemaphoreType.DMA((4,)),
        ],
        compiler_params=params(24),
        cost_estimate=cost(1 << 28, 6 << 20),
        name="rows_sum",
    )(received, arrived)


def cot_copies(half, cot_hbm, cot, sems):
    tokens, wide = cot.shape
    steps = sems.shape[0]
    block = tokens // steps
    columns = pl.ds(pl.multiple_of(half * wide, wide), wide)
    copies = []
    for i in range(steps):
        rows = pl.ds(i * block, block)
        copies.append(
            pltpu.make_async_copy(cot_hbm.at[rows, columns], cot.at[rows, :], sems.at[i])
        )
        copies[-1].start()
    return copies


def add_terms(emb, cot, i, out_ref):
    tokens = emb.shape[1]
    block = 512
    for c in range(out_ref.shape[1] // block):
        columns = slice(c * block, (c + 1) * block)
        part = dot(emb, cot[i * tokens : (i + 1) * tokens, columns])
        if i == 0:
            out_ref[:, columns] = part
        else:
            out_ref[:, columns] += part


def terms_kernel(core_ref, emb_ref, cot_hbm, out_ref, cot, sems):
    copies = cot_copies(core_ref[0], cot_hbm, cot, sems)
    block = emb_ref.shape[1] // len(copies)
    for i, copy in enumerate(copies):
        copy.wait()
        add_terms(emb_ref[:, i * block : (i + 1) * block], cot, i, out_ref)


def first_terms_kernel(
    core_ref, count_ref, slot_ref, rows_ref, cot_hbm, emb_ref, out_ref, cot, sems
):
    copies = cot_copies(1 - core_ref[0], cot_hbm, cot, sems)
    chunks, _, block = slot_ref.shape
    n, double, width = rows_ref.shape
    n_slots = n * double // 2
    across = rows_ref[:, : double // 2, :].reshape(n_slots, width).T
    step = 256
    line = lax.broadcasted_iota(jnp.int32, (step, block), 0)
    for k in range(chunks):
        slot = slot_ref[k]
        total = jnp.zeros((width, block), F32)
        for c in range(n_slots // step):
            total += dot(across[:, c * step : (c + 1) * step], one_hot(line + c * step == slot))
        token = lax.broadcasted_iota(jnp.int32, total.shape, 1) + k * block
        emb = jnp.where(token < count_ref[0], total, 0.0).astype(BF16)
        emb_ref[:, k * block : (k + 1) * block] = emb
        copies[k].wait()
        add_terms(emb, cot, k, out_ref)


def first_terms(core, counts, slots, returned, cotangent):
    tokens, hidden = cotangent.shape
    width = returned.shape[2]
    return pl.pallas_call(
        first_terms_kernel,
        in_specs=[SMEM, SMEM, VMEM, VMEM, HBM],
        out_specs=(VMEM, VMEM),
        scratch_shapes=[
            pltpu.VMEM((tokens, hidden // 2), BF16),
            pltpu.SemaphoreType.DMA((4,)),
        ],
        out_shape=(
            jax.ShapeDtypeStruct((width, tokens), BF16),
            jax.ShapeDtypeStruct((width, hidden // 2), F32),
        ),
        compiler_params=params(16),
        cost_estimate=cost(3 << 28, 6 << 20),
        name="first_terms",
    )(core, counts, slots, returned, in_hbm(cotangent))


def half_terms(core, embedded, cotangent):
    tokens, hidden = cotangent.shape
    width = embedded.shape[0]
    return pl.pallas_call(
        terms_kernel,
        in_specs=[SMEM, VMEM, HBM],
        out_specs=VMEM,
        scratch_shapes=[
            pltpu.VMEM((tokens, hidden // 2), BF16),
            pltpu.SemaphoreType.DMA((4,)),
        ],
        out_shape=jax.ShapeDtypeStruct((width, hidden // 2), F32),
        compiler_params=params(16),
        cost_estimate=cost(1 << 29, 5 << 20),
        name="half_terms",
    )(core, embedded, in_hbm(cotangent))


def parts_kernel(tiles, mine_ref, other_ref, out_ref):
    groups = mine_ref.shape[1] // (tiles * LANES)
    for g in range(mine_ref.shape[0] // 8):
        rows = slice(8 * g, 8 * g + 8)
        for j in range(groups):
            columns = slice(j * tiles * LANES, (j + 1) * tiles * LANES)
            total = mine_ref[rows, columns] + other_ref[rows, columns]
            block = [total[:, t * LANES : (t + 1) * LANES] for t in range(tiles)]
            out_ref[g * groups + j] = jnp.concatenate(block, axis=0).astype(BF16)


def chip_parts(mine, other, chips):
    rows, columns = mine.shape
    tiles = rows * columns // (8 * LANES * chips)
    return pl.pallas_call(
        functools.partial(parts_kernel, tiles),
        out_shape=jax.ShapeDtypeStruct((chips, 8 * tiles, LANES), BF16),
        in_specs=[VMEM, VMEM],
        out_specs=VMEM,
        compiler_params=params(8),
        cost_estimate=cost(1 << 24, 3 << 20),
        name="chip_parts",
    )(mine, other)


def total_kernel(parts_ref, out_ref):
    total = parts_ref[0].astype(F32)
    for p in range(1, parts_ref.shape[0]):
        total += parts_ref[p].astype(F32)
    total = total.astype(BF16)
    for p in range(out_ref.shape[0]):
        out_ref[p] = total


def chips_total(parts):
    return pl.pallas_call(
        total_kernel,
        out_shape=jax.ShapeDtypeStruct(parts.shape, BF16),
        in_specs=[VMEM],
        out_specs=VMEM,
        compiler_params=params(8),
        cost_estimate=cost(1 << 24, 1 << 20),
        name="chips_total",
    )(parts)


def result_kernel(tiles, scaling, own, core_ref, source_ref, *rest):
    out_hbm, half, sems = rest[-3:]
    core = core_ref[0] if own else 1 - core_ref[0]
    rows, wide = half.shape
    groups = wide // (tiles * LANES)
    columns = pl.ds(pl.multiple_of(core * wide, wide), wide)
    steps = sems.shape[0]
    block = rows // steps
    copies = []
    for i in range(steps):
        for g in range(i * block // 8, (i + 1) * block // 8):
            for j in range(groups):
                part = source_ref[g * groups + j].astype(F32) * scaling
                for t in range(tiles):
                    left = (j * tiles + t) * LANES
                    half[8 * g : 8 * g + 8, left : left + LANES] = part[8 * t : 8 * t + 8, :]
        lines = pl.ds(i * block, block)
        target = out_hbm.at[lines, columns]
        copies.append(pltpu.make_async_copy(half.at[lines, :], target, sems.at[i]))
        copies[-1].start()
    for copy in copies:
        copy.wait()


def result_half(own, core, source, before, width, hidden, scaling):
    tiles = source.shape[1] // 8
    steps = 4
    return pl.pallas_call(
        functools.partial(result_kernel, tiles, scaling, own),
        out_shape=jax.ShapeDtypeStruct((width, hidden), F32),
        in_specs=[SMEM, VMEM] + [HBM] * len(before),
        out_specs=HBM,
        input_output_aliases={2: 0} if before else {},
        scratch_shapes=[
            pltpu.VMEM((width, hidden // 2), F32),
            pltpu.SemaphoreType.DMA((steps,)),
        ],
        compiler_params=params(8),
        cost_estimate=cost(1 << 24, 3 << 20),
        name="own_result" if own else "result",
    )(core, source, *before)


def hidden_kernel(emb_ref, proj_ref, out_ref):
    out_ref[...] = dot(emb_ref[...].T, proj_ref[...]).astype(BF16)


def hidden_rows(embedded, projection):
    width, tokens = embedded.shape
    hidden = projection.shape[1]
    block = 256
    return pl.pallas_call(
        hidden_kernel,
        grid=(tokens // block,),
        out_shape=jax.ShapeDtypeStruct((tokens, hidden), BF16),
        in_specs=[
            pl.BlockSpec((width, block), lambda i: (0, i)),
            pl.BlockSpec((width, hidden), lambda i: (0, 0)),
        ],
        out_specs=pl.BlockSpec((block, hidden), lambda i: (i, 0)),
        compiler_params=params(16),
        cost_estimate=cost(1 << 30, 9 << 20),
        name="hidden_rows",
    )(embedded, projection)


def body(token_ids, counts, table, projection, cotangent):
    tokens = token_ids.shape[0]
    held_rows, width = table.shape
    hidden_width = projection.shape[1]
    n = lax.axis_size(ALL)
    chips = lax.axis_size(CHIPS)
    capacity = 2 * tokens // n
    core = lax.axis_index(CORE).astype(jnp.int32).reshape(1)
    slots, requests = prepare(core, counts, token_ids, held_rows, n, capacity, 256)
    received = exchange(requests.reshape(n, 1, capacity), ALL)
    outgoing, held = placed_grads(
        counts, slots, projection, cotangent, table, n * capacity
    )
    picked = picked_rows(received, outgoing, held)
    returned = exchange(picked, ALL)
    embedded, theirs = first_terms(core, counts, slots, returned, cotangent)
    other = lax.ppermute(theirs, CORE, SWAP)
    mine = half_terms(core, embedded, cotangent)
    parts = chip_parts(mine, other, chips)
    arrived = exchange(parts, CHIPS)
    hidden = hidden_rows(embedded, projection)
    total = chips_total(arrived)
    whole = exchange(total, CHIPS)
    across = lax.ppermute(whole, CORE, SWAP)
    scaling = 1.0 / math.sqrt(tokens * n)
    partial = result_half(True, core, whole, (), width, hidden_width, scaling)
    grad_projection = result_half(False, core, across, (partial,), width, hidden_width, scaling)
    grad_table = rows_sum(received, returned, held_rows)
    return (hidden, grad_projection, grad_table)


def solution(mesh):
    finer = Mesh(
        mesh.devices.reshape(4, 4, 2, mesh.shape["dp"]), ("vocab_0", "vocab_1", "vocab_2", "dp")
    )
    in_specs = (P(ALL), P(ALL), P(ALL, None), P(), P(ALL, None))
    out_specs = (P(ALL, None), P(), P(ALL, None))
    return jax.shard_map(body, mesh=finer, in_specs=in_specs, out_specs=out_specs, check_vma=False)
```

```python
import functools
import math

import jax
import jax.numpy as jnp
from jax import lax
from jax.experimental import pallas as pl
from jax.experimental.pallas import tpu as pltpu
from jax.sharding import Mesh
from jax.sharding import PartitionSpec as P


ALL = ("vocab_0", "vocab_1", "vocab_2", "dp")
CHIPS = ("vocab_0", "vocab_1", "dp")
CORE = "vocab_2"
SWAP = ((0, 1), (1, 0))
LANES = 128
BF16 = jnp.bfloat16
F32 = jnp.float32
VMEM = pl.BlockSpec(memory_space=pltpu.VMEM)
SMEM = pl.BlockSpec(memory_space=pltpu.SMEM)
HBM = pl.BlockSpec(memory_space=pltpu.HBM)


def in_hbm(x):
    return pltpu.with_memory_space_constraint(x, pltpu.HBM)


def in_vmem(x):
    return pltpu.with_memory_space_constraint(x, pltpu.VMEM)


def params(mib):
    return pltpu.CompilerParams(vmem_limit_bytes=mib << 20)


def cost(flops, nbytes):
    return pl.CostEstimate(flops=flops, bytes_accessed=nbytes, transcendentals=0)


def dot(a, b, dims=((1,), (0,))):
    return lax.dot_general(a, b, (dims, ((), ())), preferred_element_type=F32)


def one_hot(hit):
    return jnp.where(hit, 1.0, 0.0).astype(BF16)


def exchange(blocks, axes):
    return lax.all_to_all(blocks, axes, split_axis=0, concat_axis=0, tiled=True)


def prepare_kernel(
    shift, capacity, core_ref, count_ref, ids_ref, slot_ref, request_ref, hits_ref, row_ref
):
    del core_ref, count_ref
    n = request_ref.shape[0]
    chunks, lanes = ids_ref.shape
    holder = lax.broadcasted_iota(jnp.int32, (n, lanes), 0)
    line = lax.broadcasted_iota(jnp.int32, (lanes, 2 * lanes), 0)
    column = lax.broadcasted_iota(jnp.int32, (lanes, 2 * lanes), 1)
    before = one_hot(line < column)
    place = lax.broadcasted_iota(jnp.int32, (capacity, lanes), 0)
    seen = jnp.zeros((n, lanes), F32)
    ids = ids_ref[...]
    owner = lax.shift_right_logical(ids, shift)
    row = ids & ((1 << shift) - 1)
    upper = lax.shift_right_logical(row, 7).astype(F32)
    lower = (row & 127).astype(F32)
    for k in range(chunks):
        own = owner[k : k + 1, :]
        hit = holder == own
        columns = slice(k * lanes, (k + 1) * lanes)
        hits_ref[:, columns] = one_hot(hit)
        counted = dot(hits_ref[:, columns], before)
        earlier = counted[:, :lanes] + seen
        seen = seen + counted[:, lanes:]
        rank = jnp.sum(jnp.where(hit, earlier, 0.0), axis=0, keepdims=True).astype(jnp.int32)
        per = slot_ref.shape[2] // lanes
        slot_ref[k // per, :, (k % per) * lanes : (k % per + 1) * lanes] = own * capacity + rank
        mine = place == rank
        high = jnp.where(mine, upper[k : k + 1, :], 0.0)
        low = jnp.where(mine, lower[k : k + 1, :], 0.0)
        row_ref[:, columns] = jnp.concatenate([high, low], axis=0).astype(BF16)
    split = dot(hits_ref[...], row_ref[...], ((1,), (1,)))
    request_ref[...] = (split[:, :capacity] * 128.0 + split[:, capacity:]).astype(jnp.int32)


def prepare(core, counts, token_ids, held_rows, n, capacity, block):
    tokens = token_ids.shape[0]
    shift = held_rows.bit_length() - 1
    assert held_rows == 1 << shift and shift <= 15
    return pl.pallas_call(
        functools.partial(prepare_kernel, shift, capacity),
        out_shape=(
            jax.ShapeDtypeStruct((tokens // block, 1, block), jnp.int32),
            jax.ShapeDtypeStruct((n, capacity), jnp.int32),
        ),
        in_specs=[SMEM, SMEM, VMEM],
        out_specs=(VMEM, VMEM),
        scratch_shapes=[
            pltpu.VMEM((n, tokens), BF16),
            pltpu.VMEM((2 * capacity, tokens), BF16),
        ],
        compiler_params=params(8),
        cost_estimate=cost(1 << 26, 1 << 16),
        name="prepare",
    )(core, counts, token_ids.reshape(tokens // LANES, LANES))


def grads_kernel(
    count_ref, slot_ref, proj_hbm, cot_hbm, table_hbm, out_ref, table, cot, proj, across, grads, sems
):
    steps, _, block = slot_ref.shape
    proj_copy = pltpu.make_async_copy(proj_hbm, proj, sems.at[steps])
    proj_copy.start()
    copies = []
    for i in range(steps):
        rows = pl.ds(i * block, block)
        copies.append(pltpu.make_async_copy(cot_hbm.at[rows, :], cot.at[rows, :], sems.at[i]))
        copies[-1].start()
    table_copy = pltpu.make_async_copy(table_hbm, table, sems.at[steps + 1])
    table_copy.start()
    proj_copy.wait()
    across[...] = proj[...].T
    for i in range(steps):
        copies[i].wait()
        rows = slice(i * block, (i + 1) * block)
        grad = dot(cot[rows, :], across[...])
        token = lax.broadcasted_iota(jnp.int32, grad.shape, 0) + i * block
        grads[rows, :] = jnp.where(token < count_ref[0], grad, 0.0).astype(BF16)
    step = 256
    line = lax.broadcasted_iota(jnp.int32, (step, block), 0)
    for c in range(out_ref.shape[0] // step):
        total = jnp.zeros((step, out_ref.shape[1]), F32)
        for k in range(steps):
            hit = line == slot_ref[k] - c * step
            total += dot(one_hot(hit), grads[k * block : (k + 1) * block, :])
        out_ref[c * step : (c + 1) * step, :] = total.astype(BF16)
    table_copy.wait()


def placed_grads(counts, slots, projection, cotangent, table, n_slots):
    tokens, hidden = cotangent.shape
    width = projection.shape[0]
    return pl.pallas_call(
        grads_kernel,
        out_shape=(
            jax.ShapeDtypeStruct((n_slots, width), BF16),
            pltpu.VMEM(table.shape, table.dtype),
        ),
        in_specs=[SMEM, VMEM, HBM, HBM, HBM],
        out_specs=(VMEM, VMEM),
        scratch_shapes=[
            pltpu.VMEM((tokens, hidden), BF16),
            pltpu.VMEM((width, hidden), BF16),
            pltpu.VMEM((hidden, width), BF16),
            pltpu.VMEM((tokens, width), BF16),
            pltpu.SemaphoreType.DMA((slots.shape[0] + 2,)),
        ],
        compiler_params=params(24),
        cost_estimate=cost(3 << 29, 10 << 20),
        name="placed_grads",
    )(counts, slots, in_hbm(projection), in_hbm(cotangent), in_hbm(table))


def pick_kernel(index_ref, grads_ref, held_ref, out_ref, index, packed, table, stage, sem):
    n, _, capacity = index_ref.shape
    packed[...] = index_ref[...].reshape(n, capacity).T
    copy = pltpu.make_async_copy(packed, index, sem)
    copy.start()
    for p in range(n):
        out_ref[p, capacity:, :] = grads_ref[p * capacity : (p + 1) * capacity, :]
    step = 256

    @pl.loop(0, table.shape[0] // step)
    def _(c):
        rows = pl.ds(pl.multiple_of(c * step, step), step)
        table[rows, :] = held_ref[rows, :].astype(F32)

    copy.wait()
    unroll = 8

    @pl.loop(0, n // unroll)
    def _(q):
        for k in range(unroll):
            p = q * unroll + k
            for r in range(capacity):
                stage[pl.ds(p * capacity + r, 1), :] = table[pl.ds(index[r, p], 1), :]

    for p in range(n):
        out_ref[p, :capacity, :] = stage[p * capacity : (p + 1) * capacity, :].astype(BF16)


def picked_rows(received, outgoing, held):
    n, _, capacity = received.shape
    slots = n * capacity
    rows, width = held.shape
    return pl.pallas_call(
        pick_kernel,
        out_shape=jax.ShapeDtypeStruct((n, 2 * capacity, width), BF16),
        in_specs=[VMEM, VMEM, VMEM],
        out_specs=VMEM,
        scratch_shapes=[
            pltpu.SMEM((capacity, n), jnp.int32),
            pltpu.VMEM((capacity, n), jnp.int32),
            pltpu.VMEM((rows, width), F32),
            pltpu.VMEM((slots, width), F32),
            pltpu.SemaphoreType.DMA(()),
        ],
        compiler_params=params(14),
        cost_estimate=cost(1 << 26, 3 << 20),
        name="picked_rows",
    )(received, outgoing, in_vmem(held))


def rows_sum_kernel(index_ref, grads_ref, out_hbm, index, wide, first, *rest):
    *others, index_sem, sems = rest
    copy = pltpu.make_async_copy(index_ref, index, index_sem)
    copy.start()
    sums = (first, *others)
    held, width = first.shape
    step = 256

    @pl.loop(0, held // step)
    def _(c):
        rows = pl.ds(pl.multiple_of(c * step, step), step)
        for total in sums:
            total[rows, :] = jnp.zeros((step, width), F32)

    n, _, capacity = index_ref.shape
    for p in range(n):
        wide[p * capacity : (p + 1) * capacity, :] = grads_ref[p, capacity:, :].astype(F32)
    copy.wait()
    share = n // len(sums)

    @pl.loop(0, share)
    def _(q):
        for r in range(capacity):
            for s, total in enumerate(sums):
                p = q + s * share
                row = pl.ds(index[p, 0, r], 1)
                total[row, :] += wide[pl.ds(p * capacity + r, 1), :]

    steps = sems.shape[0]
    block = held // steps
    copies = []
    for i in range(steps):

        @pl.loop(i * block // step, (i + 1) * block // step)
        def _(c):
            rows = pl.ds(pl.multiple_of(c * step, step), step)
            first[rows, :] = (first[rows, :] + others[0][rows, :]) + (
                others[1][rows, :] + others[2][rows, :]
            )

        rows = pl.ds(i * block, block)
        copies.append(pltpu.make_async_copy(first.at[rows, :], out_hbm.at[rows, :], sems.at[i]))
        copies[-1].start()
    for copy in copies:
        copy.wait()


def rows_sum(received, arrived, held_rows):
    n, _, capacity = received.shape
    width = arrived.shape[2]
    total = pltpu.VMEM((held_rows, width), F32)
    return pl.pallas_call(
        rows_sum_kernel,
        out_shape=jax.ShapeDtypeStruct((held_rows, width), F32),
        in_specs=[VMEM, VMEM],
        out_specs=HBM,
        scratch_shapes=[
            pltpu.SMEM(received.shape, jnp.int32),
            pltpu.VMEM((n * capacity, width), F32),
            total,
            total,
            total,
            total,
            pltpu.SemaphoreType.DMA(()),
            pltpu.SemaphoreType.DMA((4,)),
        ],
        compiler_params=params(24),
        cost_estimate=cost(1 << 28, 6 << 20),
        name="rows_sum",
    )(received, arrived)


def cot_copies(half, cot_hbm, cot, sems):
    tokens, wide = cot.shape
    steps = sems.shape[0]
    block = tokens // steps
    columns = pl.ds(pl.multiple_of(half * wide, wide), wide)
    copies = []
    for i in range(steps):
        rows = pl.ds(i * block, block)
        copies.append(
            pltpu.make_async_copy(cot_hbm.at[rows, columns], cot.at[rows, :], sems.at[i])
        )
        copies[-1].start()
    return copies


def add_terms(emb, cot, i, out_ref):
    tokens = emb.shape[1]
    block = 512
    for c in range(out_ref.shape[1] // block):
        columns = slice(c * block, (c + 1) * block)
        part = dot(emb, cot[i * tokens : (i + 1) * tokens, columns])
        if i == 0:
            out_ref[:, columns] = part
        else:
            out_ref[:, columns] += part


def terms_kernel(core_ref, emb_ref, cot_hbm, out_ref, cot, sems):
    copies = cot_copies(core_ref[0], cot_hbm, cot, sems)
    block = emb_ref.shape[1] // len(copies)
    for i, copy in enumerate(copies):
        copy.wait()
        add_terms(emb_ref[:, i * block : (i + 1) * block], cot, i, out_ref)


def first_terms_kernel(
    core_ref, count_ref, slot_ref, rows_ref, cot_hbm, emb_ref, out_ref, cot, sems
):
    copies = cot_copies(1 - core_ref[0], cot_hbm, cot, sems)
    chunks, _, block = slot_ref.shape
    n, double, width = rows_ref.shape
    n_slots = n * double // 2
    across = rows_ref[:, : double // 2, :].reshape(n_slots, width).T
    step = 256
    line = lax.broadcasted_iota(jnp.int32, (step, block), 0)
    for k in range(chunks):
        slot = slot_ref[k]
        total = jnp.zeros((width, block), F32)
        for c in range(n_slots // step):
            total += dot(across[:, c * step : (c + 1) * step], one_hot(line + c * step == slot))
        token = lax.broadcasted_iota(jnp.int32, total.shape, 1) + k * block
        emb = jnp.where(token < count_ref[0], total, 0.0).astype(BF16)
        emb_ref[:, k * block : (k + 1) * block] = emb
        copies[k].wait()
        add_terms(emb, cot, k, out_ref)


def first_terms(core, counts, slots, returned, cotangent):
    tokens, hidden = cotangent.shape
    width = returned.shape[2]
    return pl.pallas_call(
        first_terms_kernel,
        in_specs=[SMEM, SMEM, VMEM, VMEM, HBM],
        out_specs=(VMEM, VMEM),
        scratch_shapes=[
            pltpu.VMEM((tokens, hidden // 2), BF16),
            pltpu.SemaphoreType.DMA((4,)),
        ],
        out_shape=(
            jax.ShapeDtypeStruct((width, tokens), BF16),
            jax.ShapeDtypeStruct((width, hidden // 2), F32),
        ),
        compiler_params=params(16),
        cost_estimate=cost(3 << 28, 6 << 20),
        name="first_terms",
    )(core, counts, slots, returned, in_hbm(cotangent))


def half_terms(core, embedded, cotangent):
    tokens, hidden = cotangent.shape
    width = embedded.shape[0]
    return pl.pallas_call(
        terms_kernel,
        in_specs=[SMEM, VMEM, HBM],
        out_specs=VMEM,
        scratch_shapes=[
            pltpu.VMEM((tokens, hidden // 2), BF16),
            pltpu.SemaphoreType.DMA((4,)),
        ],
        out_shape=jax.ShapeDtypeStruct((width, hidden // 2), F32),
        compiler_params=params(16),
        cost_estimate=cost(1 << 29, 5 << 20),
        name="half_terms",
    )(core, embedded, in_hbm(cotangent))


def parts_kernel(tiles, mine_ref, other_ref, out_hbm, parts, sems):
    groups = mine_ref.shape[1] // (tiles * LANES)
    steps = sems.shape[0]
    per = mine_ref.shape[0] // 8 // steps
    copies = []
    for i in range(steps):
        for g in range(i * per, (i + 1) * per):
            rows = slice(8 * g, 8 * g + 8)
            for j in range(groups):
                columns = slice(j * tiles * LANES, (j + 1) * tiles * LANES)
                total = mine_ref[rows, columns] + other_ref[rows, columns]
                block = [total[:, t * LANES : (t + 1) * LANES] for t in range(tiles)]
                parts[g * groups + j] = jnp.concatenate(block, axis=0).astype(BF16)
        chips = pl.ds(i * per * groups, per * groups)
        copies.append(pltpu.make_async_copy(parts.at[chips], out_hbm.at[chips], sems.at[i]))
        copies[-1].start()
    for copy in copies:
        copy.wait()


def chip_parts(mine, other, chips):
    rows, columns = mine.shape
    tiles = rows * columns // (8 * LANES * chips)
    return pl.pallas_call(
        functools.partial(parts_kernel, tiles),
        out_shape=jax.ShapeDtypeStruct((chips, 8 * tiles, LANES), BF16),
        in_specs=[VMEM, VMEM],
        out_specs=HBM,
        scratch_shapes=[
            pltpu.VMEM((chips, 8 * tiles, LANES), BF16),
            pltpu.SemaphoreType.DMA((4,)),
        ],
        compiler_params=params(8),
        cost_estimate=cost(1 << 24, 3 << 20),
        name="chip_parts",
    )(mine, other)


def total_kernel(parts_ref, out_ref):
    total = parts_ref[0].astype(F32)
    for p in range(1, parts_ref.shape[0]):
        total += parts_ref[p].astype(F32)
    total = total.astype(BF16)
    for p in range(out_ref.shape[0]):
        out_ref[p] = total


def chips_total(parts):
    return pl.pallas_call(
        total_kernel,
        out_shape=jax.ShapeDtypeStruct(parts.shape, BF16),
        in_specs=[VMEM],
        out_specs=VMEM,
        compiler_params=params(8),
        cost_estimate=cost(1 << 24, 1 << 20),
        name="chips_total",
    )(parts)


def result_kernel(tiles, scaling, own, core_ref, source_ref, *rest):
    out_hbm, half, sems = rest[-3:]
    core = core_ref[0] if own else 1 - core_ref[0]
    rows, wide = half.shape
    groups = wide // (tiles * LANES)
    columns = pl.ds(pl.multiple_of(core * wide, wide), wide)
    steps = sems.shape[0]
    block = rows // steps
    copies = []
    for i in range(steps):
        for g in range(i * block // 8, (i + 1) * block // 8):
            for j in range(groups):
                part = source_ref[g * groups + j].astype(F32) * scaling
                for t in range(tiles):
                    left = (j * tiles + t) * LANES
                    half[8 * g : 8 * g + 8, left : left + LANES] = part[8 * t : 8 * t + 8, :]
        lines = pl.ds(i * block, block)
        target = out_hbm.at[lines, columns]
        copies.append(pltpu.make_async_copy(half.at[lines, :], target, sems.at[i]))
        copies[-1].start()
    for copy in copies:
        copy.wait()


def result_half(own, core, source, before, width, hidden, scaling):
    tiles = source.shape[1] // 8
    steps = 4
    return pl.pallas_call(
        functools.partial(result_kernel, tiles, scaling, own),
        out_shape=jax.ShapeDtypeStruct((width, hidden), F32),
        in_specs=[SMEM, VMEM] + [HBM] * len(before),
        out_specs=HBM,
        input_output_aliases={2: 0} if before else {},
        scratch_shapes=[
            pltpu.VMEM((width, hidden // 2), F32),
            pltpu.SemaphoreType.DMA((steps,)),
        ],
        compiler_params=params(8),
        cost_estimate=cost(1 << 24, 3 << 20),
        name="own_result" if own else "result",
    )(core, source, *before)


def hidden_kernel(emb_ref, proj_ref, out_ref):
    out_ref[...] = dot(emb_ref[...].T, proj_ref[...]).astype(BF16)


def hidden_rows(embedded, projection):
    width, tokens = embedded.shape
    hidden = projection.shape[1]
    block = 256
    return pl.pallas_call(
        hidden_kernel,
        grid=(tokens // block,),
        out_shape=jax.ShapeDtypeStruct((tokens, hidden), BF16),
        in_specs=[
            pl.BlockSpec((width, block), lambda i: (0, i)),
            pl.BlockSpec((width, hidden), lambda i: (0, 0)),
        ],
        out_specs=pl.BlockSpec((block, hidden), lambda i: (i, 0)),
        compiler_params=params(16),
        cost_estimate=cost(1 << 30, 9 << 20),
        name="hidden_rows",
    )(embedded, projection)


def body(token_ids, counts, table, projection, cotangent):
    tokens = token_ids.shape[0]
    held_rows, width = table.shape
    hidden_width = projection.shape[1]
    n = lax.axis_size(ALL)
    chips = lax.axis_size(CHIPS)
    capacity = 2 * tokens // n
    core = lax.axis_index(CORE).astype(jnp.int32).reshape(1)
    slots, requests = prepare(core, counts, token_ids, held_rows, n, capacity, 256)
    received = exchange(requests.reshape(n, 1, capacity), ALL)
    outgoing, held = placed_grads(
        counts, slots, projection, cotangent, table, n * capacity
    )
    picked = picked_rows(received, outgoing, held)
    returned = exchange(picked, ALL)
    embedded, theirs = first_terms(core, counts, slots, returned, cotangent)
    other = lax.ppermute(theirs, CORE, SWAP)
    mine = half_terms(core, embedded, cotangent)
    parts = chip_parts(mine, other, chips)
    arrived = exchange(parts, CHIPS)
    hidden = hidden_rows(embedded, projection)
    total = chips_total(arrived)
    whole = exchange(total, CHIPS)
    across = lax.ppermute(whole, CORE, SWAP)
    scaling = 1.0 / math.sqrt(tokens * n)
    partial = result_half(True, core, whole, (), width, hidden_width, scaling)
    grad_projection = result_half(False, core, across, (partial,), width, hidden_width, scaling)
    grad_table = rows_sum(received, returned, held_rows)
    return (hidden, grad_projection, grad_table)


def solution(mesh):
    finer = Mesh(
        mesh.devices.reshape(4, 4, 2, mesh.shape["dp"]), ("vocab_0", "vocab_1", "vocab_2", "dp")
    )
    in_specs = (P(ALL), P(ALL), P(ALL, None), P(), P(ALL, None))
    out_specs = (P(ALL, None), P(), P(ALL, None))
    return jax.shard_map(body, mesh=finer, in_specs=in_specs, out_specs=out_specs, check_vma=False)
```

```python
import functools
import math

import jax
import jax.numpy as jnp
from jax import lax
from jax.experimental import pallas as pl
from jax.experimental.pallas import tpu as pltpu
from jax.sharding import Mesh
from jax.sharding import PartitionSpec as P


ALL = ("vocab_0", "vocab_1", "vocab_2", "dp")
CHIPS = ("vocab_0", "vocab_1", "dp")
CORE = "vocab_2"
SWAP = ((0, 1), (1, 0))
LANES = 128
BF16 = jnp.bfloat16
F32 = jnp.float32
VMEM = pl.BlockSpec(memory_space=pltpu.VMEM)
SMEM = pl.BlockSpec(memory_space=pltpu.SMEM)
HBM = pl.BlockSpec(memory_space=pltpu.HBM)


def in_hbm(x):
    return pltpu.with_memory_space_constraint(x, pltpu.HBM)


def in_vmem(x):
    return pltpu.with_memory_space_constraint(x, pltpu.VMEM)


def params(mib):
    return pltpu.CompilerParams(vmem_limit_bytes=mib << 20)


def cost(flops, nbytes):
    return pl.CostEstimate(flops=flops, bytes_accessed=nbytes, transcendentals=0)


def dot(a, b, dims=((1,), (0,))):
    return lax.dot_general(a, b, (dims, ((), ())), preferred_element_type=F32)


def one_hot(hit):
    return jnp.where(hit, 1.0, 0.0).astype(BF16)


def exchange(blocks, axes):
    return lax.all_to_all(blocks, axes, split_axis=0, concat_axis=0, tiled=True)


def prepare_kernel(
    shift, capacity, core_ref, count_ref, ids_ref, slot_ref, request_ref, hits_ref, row_ref
):
    del core_ref, count_ref
    n = request_ref.shape[0]
    chunks, lanes = ids_ref.shape
    holder = lax.broadcasted_iota(jnp.int32, (n, lanes), 0)
    line = lax.broadcasted_iota(jnp.int32, (lanes, 2 * lanes), 0)
    column = lax.broadcasted_iota(jnp.int32, (lanes, 2 * lanes), 1)
    before = one_hot(line < column)
    place = lax.broadcasted_iota(jnp.int32, (capacity, lanes), 0)
    seen = jnp.zeros((n, lanes), F32)
    ids = ids_ref[...]
    owner = lax.shift_right_logical(ids, shift)
    row = ids & ((1 << shift) - 1)
    upper = lax.shift_right_logical(row, 7).astype(F32)
    lower = (row & 127).astype(F32)
    for k in range(chunks):
        own = owner[k : k + 1, :]
        hit = holder == own
        columns = slice(k * lanes, (k + 1) * lanes)
        hits_ref[:, columns] = one_hot(hit)
        counted = dot(hits_ref[:, columns], before)
        earlier = counted[:, :lanes] + seen
        seen = seen + counted[:, lanes:]
        rank = jnp.sum(jnp.where(hit, earlier, 0.0), axis=0, keepdims=True).astype(jnp.int32)
        per = slot_ref.shape[2] // lanes
        slot_ref[k // per, :, (k % per) * lanes : (k % per + 1) * lanes] = own * capacity + rank
        mine = place == rank
        high = jnp.where(mine, upper[k : k + 1, :], 0.0)
        low = jnp.where(mine, lower[k : k + 1, :], 0.0)
        row_ref[:, columns] = jnp.concatenate([high, low], axis=0).astype(BF16)
    split = dot(hits_ref[...], row_ref[...], ((1,), (1,)))
    request_ref[...] = (split[:, :capacity] * 128.0 + split[:, capacity:]).astype(jnp.int32)


def prepare(core, counts, token_ids, held_rows, n, capacity, block):
    tokens = token_ids.shape[0]
    shift = held_rows.bit_length() - 1
    assert held_rows == 1 << shift and shift <= 15
    return pl.pallas_call(
        functools.partial(prepare_kernel, shift, capacity),
        out_shape=(
            jax.ShapeDtypeStruct((tokens // block, 1, block), jnp.int32),
            jax.ShapeDtypeStruct((n, capacity), jnp.int32),
        ),
        in_specs=[SMEM, SMEM, VMEM],
        out_specs=(VMEM, VMEM),
        scratch_shapes=[
            pltpu.VMEM((n, tokens), BF16),
            pltpu.VMEM((2 * capacity, tokens), BF16),
        ],
        compiler_params=params(8),
        cost_estimate=cost(1 << 26, 1 << 16),
        name="prepare",
    )(core, counts, token_ids.reshape(tokens // LANES, LANES))


def grads_kernel(
    count_ref, slot_ref, proj_hbm, cot_hbm, table_hbm, out_ref, table, cot, proj, across, grads, sems
):
    steps, _, block = slot_ref.shape
    proj_copy = pltpu.make_async_copy(proj_hbm, proj, sems.at[steps])
    proj_copy.start()
    copies = []
    for i in range(steps):
        rows = pl.ds(i * block, block)
        copies.append(pltpu.make_async_copy(cot_hbm.at[rows, :], cot.at[rows, :], sems.at[i]))
        copies[-1].start()
    table_copy = pltpu.make_async_copy(table_hbm, table, sems.at[steps + 1])
    table_copy.start()
    proj_copy.wait()
    across[...] = proj[...].T
    for i in range(steps):
        copies[i].wait()
        rows = slice(i * block, (i + 1) * block)
        grad = dot(cot[rows, :], across[...])
        token = lax.broadcasted_iota(jnp.int32, grad.shape, 0) + i * block
        grads[rows, :] = jnp.where(token < count_ref[0], grad, 0.0).astype(BF16)
    step = 256
    line = lax.broadcasted_iota(jnp.int32, (step, block), 0)
    for c in range(out_ref.shape[0] // step):
        total = jnp.zeros((step, out_ref.shape[1]), F32)
        for k in range(steps):
            hit = line == slot_ref[k] - c * step
            total += dot(one_hot(hit), grads[k * block : (k + 1) * block, :])
        out_ref[c * step : (c + 1) * step, :] = total.astype(BF16)
    table_copy.wait()


def placed_grads(counts, slots, projection, cotangent, table, n_slots):
    tokens, hidden = cotangent.shape
    width = projection.shape[0]
    return pl.pallas_call(
        grads_kernel,
        out_shape=(
            jax.ShapeDtypeStruct((n_slots, width), BF16),
            pltpu.VMEM(table.shape, table.dtype),
        ),
        in_specs=[SMEM, VMEM, HBM, HBM, HBM],
        out_specs=(VMEM, VMEM),
        scratch_shapes=[
            pltpu.VMEM((tokens, hidden), BF16),
            pltpu.VMEM((width, hidden), BF16),
            pltpu.VMEM((hidden, width), BF16),
            pltpu.VMEM((tokens, width), BF16),
            pltpu.SemaphoreType.DMA((slots.shape[0] + 2,)),
        ],
        compiler_params=params(24),
        cost_estimate=cost(3 << 29, 10 << 20),
        name="placed_grads",
    )(counts, slots, in_hbm(projection), in_hbm(cotangent), in_hbm(table))


def pick_kernel(index_ref, grads_ref, held_ref, out_ref, index, packed, table, stage, sem):
    n, _, capacity = index_ref.shape
    packed[...] = index_ref[...].reshape(n, capacity).T
    copy = pltpu.make_async_copy(packed, index, sem)
    copy.start()
    for p in range(n):
        out_ref[p, capacity:, :] = grads_ref[p * capacity : (p + 1) * capacity, :]
    step = 256

    @pl.loop(0, table.shape[0] // step)
    def _(c):
        rows = pl.ds(pl.multiple_of(c * step, step), step)
        table[rows, :] = held_ref[rows, :].astype(F32)

    copy.wait()
    unroll = 8

    @pl.loop(0, n // unroll)
    def _(q):
        for k in range(unroll):
            p = q * unroll + k
            for r in range(capacity):
                stage[pl.ds(p * capacity + r, 1), :] = table[pl.ds(index[r, p], 1), :]

    for p in range(n):
        out_ref[p, :capacity, :] = stage[p * capacity : (p + 1) * capacity, :].astype(BF16)


def picked_rows(received, outgoing, held):
    n, _, capacity = received.shape
    slots = n * capacity
    rows, width = held.shape
    return pl.pallas_call(
        pick_kernel,
        out_shape=jax.ShapeDtypeStruct((n, 2 * capacity, width), BF16),
        in_specs=[VMEM, VMEM, VMEM],
        out_specs=VMEM,
        scratch_shapes=[
            pltpu.SMEM((capacity, n), jnp.int32),
            pltpu.VMEM((capacity, n), jnp.int32),
            pltpu.VMEM((rows, width), F32),
            pltpu.VMEM((slots, width), F32),
            pltpu.SemaphoreType.DMA(()),
        ],
        compiler_params=params(14),
        cost_estimate=cost(1 << 26, 3 << 20),
        name="picked_rows",
    )(received, outgoing, in_vmem(held))


def rows_sum_kernel(index_ref, grads_ref, out_hbm, index, wide, first, *rest):
    *others, index_sem, sems = rest
    copy = pltpu.make_async_copy(index_ref, index, index_sem)
    copy.start()
    sums = (first, *others)
    held, width = first.shape
    step = 256

    @pl.loop(0, held // step)
    def _(c):
        rows = pl.ds(pl.multiple_of(c * step, step), step)
        for total in sums:
            total[rows, :] = jnp.zeros((step, width), F32)

    n, _, capacity = index_ref.shape
    for p in range(n):
        wide[p * capacity : (p + 1) * capacity, :] = grads_ref[p, capacity:, :].astype(F32)
    copy.wait()
    share = n // len(sums)

    @pl.loop(0, share)
    def _(q):
        for r in range(capacity):
            for s, total in enumerate(sums):
                p = q + s * share
                row = pl.ds(index[p, 0, r], 1)
                total[row, :] += wide[pl.ds(p * capacity + r, 1), :]

    steps = sems.shape[0]
    block = held // steps
    copies = []
    for i in range(steps):

        @pl.loop(i * block // step, (i + 1) * block // step)
        def _(c):
            rows = pl.ds(pl.multiple_of(c * step, step), step)
            first[rows, :] = (first[rows, :] + others[0][rows, :]) + (
                others[1][rows, :] + others[2][rows, :]
            )

        rows = pl.ds(i * block, block)
        copies.append(pltpu.make_async_copy(first.at[rows, :], out_hbm.at[rows, :], sems.at[i]))
        copies[-1].start()
    for copy in copies:
        copy.wait()


def rows_sum(received, arrived, held_rows):
    n, _, capacity = received.shape
    width = arrived.shape[2]
    total = pltpu.VMEM((held_rows, width), F32)
    return pl.pallas_call(
        rows_sum_kernel,
        out_shape=jax.ShapeDtypeStruct((held_rows, width), F32),
        in_specs=[VMEM, VMEM],
        out_specs=HBM,
        scratch_shapes=[
            pltpu.SMEM(received.shape, jnp.int32),
            pltpu.VMEM((n * capacity, width), F32),
            total,
            total,
            total,
            total,
            pltpu.SemaphoreType.DMA(()),
            pltpu.SemaphoreType.DMA((4,)),
        ],
        compiler_params=params(24),
        cost_estimate=cost(1 << 28, 6 << 20),
        name="rows_sum",
    )(received, arrived)


def cot_copies(half, cot_hbm, cot, sems):
    tokens, wide = cot.shape
    steps = sems.shape[0]
    block = tokens // steps
    columns = pl.ds(pl.multiple_of(half * wide, wide), wide)
    copies = []
    for i in range(steps):
        rows = pl.ds(i * block, block)
        copies.append(
            pltpu.make_async_copy(cot_hbm.at[rows, columns], cot.at[rows, :], sems.at[i])
        )
        copies[-1].start()
    return copies


def add_terms(emb, cot, i, out_ref):
    tokens = emb.shape[1]
    block = 512
    for c in range(out_ref.shape[1] // block):
        columns = slice(c * block, (c + 1) * block)
        part = dot(emb, cot[i * tokens : (i + 1) * tokens, columns])
        if i == 0:
            out_ref[:, columns] = part
        else:
            out_ref[:, columns] += part


def terms_kernel(core_ref, emb_ref, cot_hbm, out_ref, cot, sems):
    copies = cot_copies(core_ref[0], cot_hbm, cot, sems)
    block = emb_ref.shape[1] // len(copies)
    for i, copy in enumerate(copies):
        copy.wait()
        add_terms(emb_ref[:, i * block : (i + 1) * block], cot, i, out_ref)


def first_terms_kernel(
    core_ref, count_ref, slot_ref, rows_ref, cot_hbm, emb_ref, out_ref, cot, sems
):
    copies = cot_copies(1 - core_ref[0], cot_hbm, cot, sems)
    chunks, _, block = slot_ref.shape
    n, double, width = rows_ref.shape
    n_slots = n * double // 2
    across = rows_ref[:, : double // 2, :].reshape(n_slots, width).T
    step = 256
    line = lax.broadcasted_iota(jnp.int32, (step, block), 0)
    for k in range(chunks):
        slot = slot_ref[k]
        total = jnp.zeros((width, block), F32)
        for c in range(n_slots // step):
            total += dot(across[:, c * step : (c + 1) * step], one_hot(line + c * step == slot))
        token = lax.broadcasted_iota(jnp.int32, total.shape, 1) + k * block
        emb = jnp.where(token < count_ref[0], total, 0.0).astype(BF16)
        emb_ref[:, k * block : (k + 1) * block] = emb
        copies[k].wait()
        add_terms(emb, cot, k, out_ref)


def first_terms(core, counts, slots, returned, cotangent):
    tokens, hidden = cotangent.shape
    width = returned.shape[2]
    return pl.pallas_call(
        first_terms_kernel,
        in_specs=[SMEM, SMEM, VMEM, VMEM, HBM],
        out_specs=(VMEM, VMEM),
        scratch_shapes=[
            pltpu.VMEM((tokens, hidden // 2), BF16),
            pltpu.SemaphoreType.DMA((4,)),
        ],
        out_shape=(
            jax.ShapeDtypeStruct((width, tokens), BF16),
            jax.ShapeDtypeStruct((width, hidden // 2), F32),
        ),
        compiler_params=params(16),
        cost_estimate=cost(3 << 28, 6 << 20),
        name="first_terms",
    )(core, counts, slots, returned, in_hbm(cotangent))


def half_terms(core, embedded, cotangent):
    tokens, hidden = cotangent.shape
    width = embedded.shape[0]
    return pl.pallas_call(
        terms_kernel,
        in_specs=[SMEM, VMEM, HBM],
        out_specs=VMEM,
        scratch_shapes=[
            pltpu.VMEM((tokens, hidden // 2), BF16),
            pltpu.SemaphoreType.DMA((4,)),
        ],
        out_shape=jax.ShapeDtypeStruct((width, hidden // 2), F32),
        compiler_params=params(16),
        cost_estimate=cost(1 << 29, 5 << 20),
        name="half_terms",
    )(core, embedded, in_hbm(cotangent))


def parts_kernel(tiles, mine_ref, other_ref, out_hbm, parts, sems):
    groups = mine_ref.shape[1] // (tiles * LANES)
    steps = sems.shape[0]
    per = mine_ref.shape[0] // 8 // steps
    copies = []
    for i in range(steps):
        for g in range(i * per, (i + 1) * per):
            rows = slice(8 * g, 8 * g + 8)
            for j in range(groups):
                columns = slice(j * tiles * LANES, (j + 1) * tiles * LANES)
                total = mine_ref[rows, columns] + other_ref[rows, columns]
                block = [total[:, t * LANES : (t + 1) * LANES] for t in range(tiles)]
                parts[g * groups + j] = jnp.concatenate(block, axis=0).astype(BF16)
        chips = pl.ds(i * per * groups, per * groups)
        copies.append(pltpu.make_async_copy(parts.at[chips], out_hbm.at[chips], sems.at[i]))
        copies[-1].start()
    for copy in copies:
        copy.wait()


def chip_parts(mine, other, chips):
    rows, columns = mine.shape
    tiles = rows * columns // (8 * LANES * chips)
    return pl.pallas_call(
        functools.partial(parts_kernel, tiles),
        out_shape=jax.ShapeDtypeStruct((chips, 8 * tiles, LANES), BF16),
        in_specs=[VMEM, VMEM],
        out_specs=HBM,
        scratch_shapes=[
            pltpu.VMEM((chips, 8 * tiles, LANES), BF16),
            pltpu.SemaphoreType.DMA((4,)),
        ],
        compiler_params=params(8),
        cost_estimate=cost(1 << 24, 3 << 20),
        name="chip_parts",
    )(mine, other)


def total_kernel(parts_ref, out_hbm, total_ref, sems):
    total = parts_ref[0].astype(F32)
    for p in range(1, parts_ref.shape[0]):
        total += parts_ref[p].astype(F32)
    total_ref[...] = total.astype(BF16)
    copies = [
        pltpu.make_async_copy(total_ref, out_hbm.at[p], sems.at[p])
        for p in range(out_hbm.shape[0])
    ]
    for copy in copies:
        copy.start()
    for copy in copies:
        copy.wait()


def chips_total(parts):
    return pl.pallas_call(
        total_kernel,
        out_shape=jax.ShapeDtypeStruct(parts.shape, BF16),
        in_specs=[VMEM],
        out_specs=HBM,
        scratch_shapes=[
            pltpu.VMEM(parts.shape[1:], BF16),
            pltpu.SemaphoreType.DMA((parts.shape[0],)),
        ],
        compiler_params=params(8),
        cost_estimate=cost(1 << 24, 1 << 20),
        name="chips_total",
    )(parts)


def result_kernel(tiles, scaling, own, core_ref, source_ref, *rest):
    out_hbm, half, sems = rest[-3:]
    core = core_ref[0] if own else 1 - core_ref[0]
    rows, wide = half.shape
    groups = wide // (tiles * LANES)
    columns = pl.ds(pl.multiple_of(core * wide, wide), wide)
    steps = sems.shape[0]
    block = rows // steps
    copies = []
    for i in range(steps):
        for g in range(i * block // 8, (i + 1) * block // 8):
            for j in range(groups):
                part = source_ref[g * groups + j].astype(F32) * scaling
                for t in range(tiles):
                    left = (j * tiles + t) * LANES
                    half[8 * g : 8 * g + 8, left : left + LANES] = part[8 * t : 8 * t + 8, :]
        lines = pl.ds(i * block, block)
        target = out_hbm.at[lines, columns]
        copies.append(pltpu.make_async_copy(half.at[lines, :], target, sems.at[i]))
        copies[-1].start()
    for copy in copies:
        copy.wait()


def result_half(own, core, source, before, width, hidden, scaling):
    tiles = source.shape[1] // 8
    steps = 4
    return pl.pallas_call(
        functools.partial(result_kernel, tiles, scaling, own),
        out_shape=jax.ShapeDtypeStruct((width, hidden), F32),
        in_specs=[SMEM, VMEM] + [HBM] * len(before),
        out_specs=HBM,
        input_output_aliases={2: 0} if before else {},
        scratch_shapes=[
            pltpu.VMEM((width, hidden // 2), F32),
            pltpu.SemaphoreType.DMA((steps,)),
        ],
        compiler_params=params(8),
        cost_estimate=cost(1 << 24, 3 << 20),
        name="own_result" if own else "result",
    )(core, source, *before)


def hidden_kernel(emb_ref, proj_ref, out_ref):
    out_ref[...] = dot(emb_ref[...].T, proj_ref[...]).astype(BF16)


def hidden_rows(embedded, projection):
    width, tokens = embedded.shape
    hidden = projection.shape[1]
    block = 256
    return pl.pallas_call(
        hidden_kernel,
        grid=(tokens // block,),
        out_shape=jax.ShapeDtypeStruct((tokens, hidden), BF16),
        in_specs=[
            pl.BlockSpec((width, block), lambda i: (0, i)),
            pl.BlockSpec((width, hidden), lambda i: (0, 0)),
        ],
        out_specs=pl.BlockSpec((block, hidden), lambda i: (i, 0)),
        compiler_params=params(16),
        cost_estimate=cost(1 << 30, 9 << 20),
        name="hidden_rows",
    )(embedded, projection)


def body(token_ids, counts, table, projection, cotangent):
    tokens = token_ids.shape[0]
    held_rows, width = table.shape
    hidden_width = projection.shape[1]
    n = lax.axis_size(ALL)
    chips = lax.axis_size(CHIPS)
    capacity = 2 * tokens // n
    core = lax.axis_index(CORE).astype(jnp.int32).reshape(1)
    slots, requests = prepare(core, counts, token_ids, held_rows, n, capacity, 256)
    received = exchange(requests.reshape(n, 1, capacity), ALL)
    outgoing, held = placed_grads(
        counts, slots, projection, cotangent, table, n * capacity
    )
    picked = picked_rows(received, outgoing, held)
    returned = exchange(picked, ALL)
    embedded, theirs = first_terms(core, counts, slots, returned, cotangent)
    other = lax.ppermute(theirs, CORE, SWAP)
    mine = half_terms(core, embedded, cotangent)
    parts = chip_parts(mine, other, chips)
    arrived = exchange(parts, CHIPS)
    hidden = hidden_rows(embedded, projection)
    total = chips_total(arrived)
    whole = exchange(total, CHIPS)
    across = lax.ppermute(whole, CORE, SWAP)
    scaling = 1.0 / math.sqrt(tokens * n)
    partial = result_half(True, core, whole, (), width, hidden_width, scaling)
    grad_projection = result_half(False, core, across, (partial,), width, hidden_width, scaling)
    grad_table = rows_sum(received, returned, held_rows)
    return (hidden, grad_projection, grad_table)


def solution(mesh):
    finer = Mesh(
        mesh.devices.reshape(4, 4, 2, mesh.shape["dp"]), ("vocab_0", "vocab_1", "vocab_2", "dp")
    )
    in_specs = (P(ALL), P(ALL), P(ALL, None), P(), P(ALL, None))
    out_specs = (P(ALL, None), P(), P(ALL, None))
    return jax.shard_map(body, mesh=finer, in_specs=in_specs, out_specs=out_specs, check_vma=False)
```

```python
import functools
import math

import jax
import jax.numpy as jnp
from jax import lax
from jax.experimental import pallas as pl
from jax.experimental.pallas import tpu as pltpu
from jax.sharding import Mesh
from jax.sharding import PartitionSpec as P


ALL = ("vocab_0", "vocab_1", "vocab_2", "dp")
CHIPS = ("vocab_0", "vocab_1", "dp")
CORE = "vocab_2"
SWAP = ((0, 1), (1, 0))
LANES = 128
BF16 = jnp.bfloat16
F32 = jnp.float32
VMEM = pl.BlockSpec(memory_space=pltpu.VMEM)
SMEM = pl.BlockSpec(memory_space=pltpu.SMEM)
HBM = pl.BlockSpec(memory_space=pltpu.HBM)


def in_hbm(x):
    return pltpu.with_memory_space_constraint(x, pltpu.HBM)


def in_vmem(x):
    return pltpu.with_memory_space_constraint(x, pltpu.VMEM)


def params(mib):
    return pltpu.CompilerParams(vmem_limit_bytes=mib << 20)


def cost(flops, nbytes):
    return pl.CostEstimate(flops=flops, bytes_accessed=nbytes, transcendentals=0)


def dot(a, b, dims=((1,), (0,))):
    return lax.dot_general(a, b, (dims, ((), ())), preferred_element_type=F32)


def one_hot(hit):
    return jnp.where(hit, 1.0, 0.0).astype(BF16)


def exchange(blocks, axes):
    return lax.all_to_all(blocks, axes, split_axis=0, concat_axis=0, tiled=True)


def prepare_kernel(
    shift, capacity, core_ref, count_ref, ids_ref, slot_ref, request_ref, hits_ref, row_ref
):
    del core_ref, count_ref
    n = request_ref.shape[0]
    chunks, lanes = ids_ref.shape
    holder = lax.broadcasted_iota(jnp.int32, (n, lanes), 0)
    line = lax.broadcasted_iota(jnp.int32, (lanes, 2 * lanes), 0)
    column = lax.broadcasted_iota(jnp.int32, (lanes, 2 * lanes), 1)
    before = one_hot(line < column)
    place = lax.broadcasted_iota(jnp.int32, (capacity, lanes), 0)
    seen = jnp.zeros((n, lanes), F32)
    ids = ids_ref[...]
    owner = lax.shift_right_logical(ids, shift)
    row = ids & ((1 << shift) - 1)
    upper = lax.shift_right_logical(row, 7).astype(F32)
    lower = (row & 127).astype(F32)
    for k in range(chunks):
        own = owner[k : k + 1, :]
        hit = holder == own
        columns = slice(k * lanes, (k + 1) * lanes)
        hits_ref[:, columns] = one_hot(hit)
        counted = dot(hits_ref[:, columns], before)
        earlier = counted[:, :lanes] + seen
        seen = seen + counted[:, lanes:]
        rank = jnp.sum(jnp.where(hit, earlier, 0.0), axis=0, keepdims=True).astype(jnp.int32)
        per = slot_ref.shape[2] // lanes
        slot_ref[k // per, :, (k % per) * lanes : (k % per + 1) * lanes] = own * capacity + rank
        mine = place == rank
        high = jnp.where(mine, upper[k : k + 1, :], 0.0)
        low = jnp.where(mine, lower[k : k + 1, :], 0.0)
        row_ref[:, columns] = jnp.concatenate([high, low], axis=0).astype(BF16)
    split = dot(hits_ref[...], row_ref[...], ((1,), (1,)))
    request_ref[...] = (split[:, :capacity] * 128.0 + split[:, capacity:]).astype(jnp.int32)


def prepare(core, counts, token_ids, held_rows, n, capacity, block):
    tokens = token_ids.shape[0]
    shift = held_rows.bit_length() - 1
    assert held_rows == 1 << shift and shift <= 15
    return pl.pallas_call(
        functools.partial(prepare_kernel, shift, capacity),
        out_shape=(
            jax.ShapeDtypeStruct((tokens // block, 1, block), jnp.int32),
            jax.ShapeDtypeStruct((n, capacity), jnp.int32),
        ),
        in_specs=[SMEM, SMEM, VMEM],
        out_specs=(VMEM, VMEM),
        scratch_shapes=[
            pltpu.VMEM((n, tokens), BF16),
            pltpu.VMEM((2 * capacity, tokens), BF16),
        ],
        compiler_params=params(8),
        cost_estimate=cost(1 << 26, 1 << 16),
        name="prepare",
    )(core, counts, token_ids.reshape(tokens // LANES, LANES))


def grads_kernel(
    count_ref, slot_ref, proj_hbm, cot_hbm, table_hbm, out_ref, table, cot, proj, across, grads, sems
):
    steps, _, block = slot_ref.shape
    proj_copy = pltpu.make_async_copy(proj_hbm, proj, sems.at[steps])
    proj_copy.start()
    copies = []
    for i in range(steps):
        rows = pl.ds(i * block, block)
        copies.append(pltpu.make_async_copy(cot_hbm.at[rows, :], cot.at[rows, :], sems.at[i]))
        copies[-1].start()
    table_copy = pltpu.make_async_copy(table_hbm, table, sems.at[steps + 1])
    table_copy.start()
    proj_copy.wait()
    across[...] = proj[...].T
    for i in range(steps):
        copies[i].wait()
        rows = slice(i * block, (i + 1) * block)
        grad = dot(cot[rows, :], across[...])
        token = lax.broadcasted_iota(jnp.int32, grad.shape, 0) + i * block
        grads[rows, :] = jnp.where(token < count_ref[0], grad, 0.0).astype(BF16)
    step = 256
    line = lax.broadcasted_iota(jnp.int32, (step, block), 0)
    for c in range(out_ref.shape[0] // step):
        total = jnp.zeros((step, out_ref.shape[1]), F32)
        for k in range(steps):
            hit = line == slot_ref[k] - c * step
            total += dot(one_hot(hit), grads[k * block : (k + 1) * block, :])
        out_ref[c * step : (c + 1) * step, :] = total.astype(BF16)
    table_copy.wait()


def placed_grads(counts, slots, projection, cotangent, table, n_slots):
    tokens, hidden = cotangent.shape
    width = projection.shape[0]
    return pl.pallas_call(
        grads_kernel,
        out_shape=(
            jax.ShapeDtypeStruct((n_slots, width), BF16),
            pltpu.VMEM(table.shape, table.dtype),
        ),
        in_specs=[SMEM, VMEM, HBM, HBM, HBM],
        out_specs=(VMEM, VMEM),
        scratch_shapes=[
            pltpu.VMEM((tokens, hidden), BF16),
            pltpu.VMEM((width, hidden), BF16),
            pltpu.VMEM((hidden, width), BF16),
            pltpu.VMEM((tokens, width), BF16),
            pltpu.SemaphoreType.DMA((slots.shape[0] + 2,)),
        ],
        compiler_params=params(24),
        cost_estimate=cost(3 << 29, 10 << 20),
        name="placed_grads",
    )(counts, slots, in_hbm(projection), in_hbm(cotangent), in_hbm(table))


def pick_kernel(index_ref, grads_ref, held_ref, out_ref, index, packed, table, stage, sem):
    n, _, capacity = index_ref.shape
    packed[...] = index_ref[...].reshape(n, capacity).T
    copy = pltpu.make_async_copy(packed, index, sem)
    copy.start()
    for p in range(n):
        out_ref[p, capacity:, :] = grads_ref[p * capacity : (p + 1) * capacity, :]
    step = 256

    @pl.loop(0, table.shape[0] // step)
    def _(c):
        rows = pl.ds(pl.multiple_of(c * step, step), step)
        table[rows, :] = held_ref[rows, :].astype(F32)

    copy.wait()
    unroll = 8

    @pl.loop(0, n // unroll)
    def _(q):
        for k in range(unroll):
            p = q * unroll + k
            for r in range(capacity):
                stage[pl.ds(p * capacity + r, 1), :] = table[pl.ds(index[r, p], 1), :]

    for p in range(n):
        out_ref[p, :capacity, :] = stage[p * capacity : (p + 1) * capacity, :].astype(BF16)


def picked_rows(received, outgoing, held):
    n, _, capacity = received.shape
    slots = n * capacity
    rows, width = held.shape
    return pl.pallas_call(
        pick_kernel,
        out_shape=jax.ShapeDtypeStruct((n, 2 * capacity, width), BF16),
        in_specs=[VMEM, VMEM, VMEM],
        out_specs=VMEM,
        scratch_shapes=[
            pltpu.SMEM((capacity, n), jnp.int32),
            pltpu.VMEM((capacity, n), jnp.int32),
            pltpu.VMEM((rows, width), F32),
            pltpu.VMEM((slots, width), F32),
            pltpu.SemaphoreType.DMA(()),
        ],
        compiler_params=params(14),
        cost_estimate=cost(1 << 26, 3 << 20),
        name="picked_rows",
    )(received, outgoing, in_vmem(held))


def rows_sum_kernel(index_ref, grads_ref, out_hbm, index, wide, first, *rest):
    *others, index_sem, sems = rest
    copy = pltpu.make_async_copy(index_ref, index, index_sem)
    copy.start()
    sums = (first, *others)
    held, width = first.shape
    step = 256

    @pl.loop(0, held // step)
    def _(c):
        rows = pl.ds(pl.multiple_of(c * step, step), step)
        for total in sums:
            total[rows, :] = jnp.zeros((step, width), F32)

    n, _, capacity = index_ref.shape
    for p in range(n):
        wide[p * capacity : (p + 1) * capacity, :] = grads_ref[p, capacity:, :].astype(F32)
    copy.wait()
    share = n // len(sums)

    @pl.loop(0, share)
    def _(q):
        for r in range(capacity):
            for s, total in enumerate(sums):
                p = q + s * share
                row = pl.ds(index[p, 0, r], 1)
                total[row, :] += wide[pl.ds(p * capacity + r, 1), :]

    steps = sems.shape[0]
    block = held // steps
    copies = []
    for i in range(steps):

        @pl.loop(i * block // step, (i + 1) * block // step)
        def _(c):
            rows = pl.ds(pl.multiple_of(c * step, step), step)
            first[rows, :] = (first[rows, :] + others[0][rows, :]) + (
                others[1][rows, :] + others[2][rows, :]
            )

        rows = pl.ds(i * block, block)
        copies.append(pltpu.make_async_copy(first.at[rows, :], out_hbm.at[rows, :], sems.at[i]))
        copies[-1].start()
    for copy in copies:
        copy.wait()


def rows_sum(received, arrived, held_rows):
    n, _, capacity = received.shape
    width = arrived.shape[2]
    total = pltpu.VMEM((held_rows, width), F32)
    return pl.pallas_call(
        rows_sum_kernel,
        out_shape=jax.ShapeDtypeStruct((held_rows, width), F32),
        in_specs=[VMEM, VMEM],
        out_specs=HBM,
        scratch_shapes=[
            pltpu.SMEM(received.shape, jnp.int32),
            pltpu.VMEM((n * capacity, width), F32),
            total,
            total,
            total,
            total,
            pltpu.SemaphoreType.DMA(()),
            pltpu.SemaphoreType.DMA((4,)),
        ],
        compiler_params=params(24),
        cost_estimate=cost(1 << 28, 6 << 20),
        name="rows_sum",
    )(received, arrived)


def cot_copies(half, cot_hbm, cot, sems):
    tokens, wide = cot.shape
    steps = sems.shape[0]
    block = tokens // steps
    columns = pl.ds(pl.multiple_of(half * wide, wide), wide)
    copies = []
    for i in range(steps):
        rows = pl.ds(i * block, block)
        copies.append(
            pltpu.make_async_copy(cot_hbm.at[rows, columns], cot.at[rows, :], sems.at[i])
        )
        copies[-1].start()
    return copies


def add_terms(emb, cot, i, out_ref):
    tokens = emb.shape[1]
    block = 512
    for c in range(out_ref.shape[1] // block):
        columns = slice(c * block, (c + 1) * block)
        part = dot(emb, cot[i * tokens : (i + 1) * tokens, columns])
        if i == 0:
            out_ref[:, columns] = part
        else:
            out_ref[:, columns] += part


def terms_kernel(core_ref, emb_ref, cot_hbm, out_ref, cot, sems):
    copies = cot_copies(core_ref[0], cot_hbm, cot, sems)
    block = emb_ref.shape[1] // len(copies)
    for i, copy in enumerate(copies):
        copy.wait()
        add_terms(emb_ref[:, i * block : (i + 1) * block], cot, i, out_ref)


def first_terms_kernel(
    core_ref, count_ref, slot_ref, rows_ref, cot_hbm, emb_ref, out_ref, cot, sems
):
    copies = cot_copies(1 - core_ref[0], cot_hbm, cot, sems)
    chunks, _, block = slot_ref.shape
    n, double, width = rows_ref.shape
    n_slots = n * double // 2
    across = rows_ref[:, : double // 2, :].reshape(n_slots, width).T
    step = 256
    line = lax.broadcasted_iota(jnp.int32, (step, block), 0)
    for k in range(chunks):
        slot = slot_ref[k]
        total = jnp.zeros((width, block), F32)
        for c in range(n_slots // step):
            total += dot(across[:, c * step : (c + 1) * step], one_hot(line + c * step == slot))
        token = lax.broadcasted_iota(jnp.int32, total.shape, 1) + k * block
        emb = jnp.where(token < count_ref[0], total, 0.0).astype(BF16)
        emb_ref[:, k * block : (k + 1) * block] = emb
        copies[k].wait()
        add_terms(emb, cot, k, out_ref)


def first_terms(core, counts, slots, returned, cotangent):
    tokens, hidden = cotangent.shape
    width = returned.shape[2]
    return pl.pallas_call(
        first_terms_kernel,
        in_specs=[SMEM, SMEM, VMEM, VMEM, HBM],
        out_specs=(VMEM, VMEM),
        scratch_shapes=[
            pltpu.VMEM((tokens, hidden // 2), BF16),
            pltpu.SemaphoreType.DMA((4,)),
        ],
        out_shape=(
            jax.ShapeDtypeStruct((width, tokens), BF16),
            jax.ShapeDtypeStruct((width, hidden // 2), F32),
        ),
        compiler_params=params(16),
        cost_estimate=cost(3 << 28, 6 << 20),
        name="first_terms",
    )(core, counts, slots, returned, in_hbm(cotangent))


def half_terms(core, embedded, cotangent):
    tokens, hidden = cotangent.shape
    width = embedded.shape[0]
    return pl.pallas_call(
        terms_kernel,
        in_specs=[SMEM, VMEM, HBM],
        out_specs=VMEM,
        scratch_shapes=[
            pltpu.VMEM((tokens, hidden // 2), BF16),
            pltpu.SemaphoreType.DMA((4,)),
        ],
        out_shape=jax.ShapeDtypeStruct((width, hidden // 2), F32),
        compiler_params=params(16),
        cost_estimate=cost(1 << 29, 5 << 20),
        name="half_terms",
    )(core, embedded, in_hbm(cotangent))


def parts_kernel(tiles, mine_ref, other_ref, out_hbm, parts, sems):
    groups = mine_ref.shape[1] // (tiles * LANES)
    steps = sems.shape[0]
    per = mine_ref.shape[0] // 8 // steps
    copies = []
    for i in range(steps):
        for g in range(i * per, (i + 1) * per):
            rows = slice(8 * g, 8 * g + 8)
            for j in range(groups):
                columns = slice(j * tiles * LANES, (j + 1) * tiles * LANES)
                total = mine_ref[rows, columns] + other_ref[rows, columns]
                block = [total[:, t * LANES : (t + 1) * LANES] for t in range(tiles)]
                parts[g * groups + j] = jnp.concatenate(block, axis=0).astype(BF16)
        chips = pl.ds(i * per * groups, per * groups)
        copies.append(pltpu.make_async_copy(parts.at[chips], out_hbm.at[chips], sems.at[i]))
        copies[-1].start()
    for copy in copies:
        copy.wait()


def chip_parts(mine, other, chips):
    rows, columns = mine.shape
    tiles = rows * columns // (8 * LANES * chips)
    return pl.pallas_call(
        functools.partial(parts_kernel, tiles),
        out_shape=jax.ShapeDtypeStruct((chips, 8 * tiles, LANES), BF16),
        in_specs=[VMEM, VMEM],
        out_specs=HBM,
        scratch_shapes=[
            pltpu.VMEM((chips, 8 * tiles, LANES), BF16),
            pltpu.SemaphoreType.DMA((4,)),
        ],
        compiler_params=params(8),
        cost_estimate=cost(1 << 24, 3 << 20),
        name="chip_parts",
    )(mine, other)


def total_kernel(parts_ref, out_hbm, total_ref, sems):
    total = parts_ref[0].astype(F32)
    for p in range(1, parts_ref.shape[0]):
        total += parts_ref[p].astype(F32)
    total = total.astype(BF16)
    several = total_ref.shape[0]
    for p in range(several):
        total_ref[p] = total
    copies = [
        pltpu.make_async_copy(total_ref, out_hbm.at[pl.ds(i * several, several)], sems.at[i])
        for i in range(out_hbm.shape[0] // several)
    ]
    for copy in copies:
        copy.start()
    for copy in copies:
        copy.wait()


def chips_total(parts):
    return pl.pallas_call(
        total_kernel,
        out_shape=jax.ShapeDtypeStruct(parts.shape, BF16),
        in_specs=[VMEM],
        out_specs=HBM,
        scratch_shapes=[
            pltpu.VMEM((parts.shape[0] // 4, *parts.shape[1:]), BF16),
            pltpu.SemaphoreType.DMA((4,)),
        ],
        compiler_params=params(8),
        cost_estimate=cost(1 << 24, 1 << 20),
        name="chips_total",
    )(parts)


def result_kernel(tiles, scaling, own, core_ref, source_ref, *rest):
    out_hbm, half, sems = rest[-3:]
    core = core_ref[0] if own else 1 - core_ref[0]
    rows, wide = half.shape
    groups = wide // (tiles * LANES)
    columns = pl.ds(pl.multiple_of(core * wide, wide), wide)
    steps = sems.shape[0]
    block = rows // steps
    copies = []
    for i in range(steps):
        for g in range(i * block // 8, (i + 1) * block // 8):
            for j in range(groups):
                part = source_ref[g * groups + j].astype(F32) * scaling
                for t in range(tiles):
                    left = (j * tiles + t) * LANES
                    half[8 * g : 8 * g + 8, left : left + LANES] = part[8 * t : 8 * t + 8, :]
        lines = pl.ds(i * block, block)
        target = out_hbm.at[lines, columns]
        copies.append(pltpu.make_async_copy(half.at[lines, :], target, sems.at[i]))
        copies[-1].start()
    for copy in copies:
        copy.wait()


def result_half(own, core, source, before, width, hidden, scaling):
    tiles = source.shape[1] // 8
    steps = 4
    return pl.pallas_call(
        functools.partial(result_kernel, tiles, scaling, own),
        out_shape=jax.ShapeDtypeStruct((width, hidden), F32),
        in_specs=[SMEM, VMEM] + [HBM] * len(before),
        out_specs=HBM,
        input_output_aliases={2: 0} if before else {},
        scratch_shapes=[
            pltpu.VMEM((width, hidden // 2), F32),
            pltpu.SemaphoreType.DMA((steps,)),
        ],
        compiler_params=params(8),
        cost_estimate=cost(1 << 24, 3 << 20),
        name="own_result" if own else "result",
    )(core, source, *before)


def hidden_kernel(emb_ref, proj_ref, out_ref):
    out_ref[...] = dot(emb_ref[...].T, proj_ref[...]).astype(BF16)


def hidden_rows(embedded, projection):
    width, tokens = embedded.shape
    hidden = projection.shape[1]
    block = 256
    return pl.pallas_call(
        hidden_kernel,
        grid=(tokens // block,),
        out_shape=jax.ShapeDtypeStruct((tokens, hidden), BF16),
        in_specs=[
            pl.BlockSpec((width, block), lambda i: (0, i)),
            pl.BlockSpec((width, hidden), lambda i: (0, 0)),
        ],
        out_specs=pl.BlockSpec((block, hidden), lambda i: (i, 0)),
        compiler_params=params(16),
        cost_estimate=cost(1 << 30, 9 << 20),
        name="hidden_rows",
    )(embedded, projection)


def body(token_ids, counts, table, projection, cotangent):
    tokens = token_ids.shape[0]
    held_rows, width = table.shape
    hidden_width = projection.shape[1]
    n = lax.axis_size(ALL)
    chips = lax.axis_size(CHIPS)
    capacity = 2 * tokens // n
    core = lax.axis_index(CORE).astype(jnp.int32).reshape(1)
    slots, requests = prepare(core, counts, token_ids, held_rows, n, capacity, 256)
    received = exchange(requests.reshape(n, 1, capacity), ALL)
    outgoing, held = placed_grads(
        counts, slots, projection, cotangent, table, n * capacity
    )
    picked = picked_rows(received, outgoing, held)
    returned = exchange(picked, ALL)
    embedded, theirs = first_terms(core, counts, slots, returned, cotangent)
    other = lax.ppermute(theirs, CORE, SWAP)
    mine = half_terms(core, embedded, cotangent)
    parts = chip_parts(mine, other, chips)
    arrived = exchange(parts, CHIPS)
    hidden = hidden_rows(embedded, projection)
    total = chips_total(arrived)
    whole = exchange(total, CHIPS)
    across = lax.ppermute(whole, CORE, SWAP)
    scaling = 1.0 / math.sqrt(tokens * n)
    partial = result_half(True, core, whole, (), width, hidden_width, scaling)
    grad_projection = result_half(False, core, across, (partial,), width, hidden_width, scaling)
    grad_table = rows_sum(received, returned, held_rows)
    return (hidden, grad_projection, grad_table)


def solution(mesh):
    finer = Mesh(
        mesh.devices.reshape(4, 4, 2, mesh.shape["dp"]), ("vocab_0", "vocab_1", "vocab_2", "dp")
    )
    in_specs = (P(ALL), P(ALL), P(ALL, None), P(), P(ALL, None))
    out_specs = (P(ALL, None), P(), P(ALL, None))
    return jax.shard_map(body, mesh=finer, in_specs=in_specs, out_specs=out_specs, check_vma=False)
```
